256 devices in a mesh: gx: 8 (over z_hi, core), gy: 4 (over x), gz: 8 (over z_lo, y).
Axes of the slice: x: 4, y: 4, z: 8 (z_hi: 4, z_lo: 2; z = z_hi * 2 + z_lo), core: 2. Of those that a mesh axis runs over, the one named last changes fastest.
Arguments:
- right_side: float32 [3, 128, 64, 1024], P(None, 'gx', 'gy', 'gz'), may hold values from -64 to 64
- damage: int32 [128, 64, 1024], P('gx', 'gy', 'gz'), may hold values from 0 to 15
Outputs:
- displacement: float32 [3, 128, 64, 1024], P(None, 'gx', 'gy', 'gz')
- norms: float32 [2], replicated
The draws below stay inside these ranges and needn't reach their ends.
All inputs are finite; a program needn't handle non-finite values.
Results may differ from the reference program's by a relative error of at most 0.0003.
Values sent between devices are 32-bit elements; how exact they have to be, the bound alone decides.
No kernel may reach another device: no remote copies, remote signals or barrier semaphores. Data moves between devices by JAX's collectives and lax.ppermute only.
A program may use at most 64 MiB of HBM per device.

```python
import math
import jax
import jax.numpy as jnp
from jax import lax

BLOCK = 16
COARSE = 8
NX = 128
NY = 64
NZ = 1024


def draw_right_side(key, part):
    key_noise = jax.random.fold_in(key, 11)
    key_rows = jax.random.fold_in(key, 12)
    key_cols = jax.random.fold_in(key, 13)
    ramp = 1.0 + 2.0 * jnp.arange(NX, dtype=jnp.float32) / NX
    rough_rows = jnp.exp(jax.random.uniform(key_rows, (NX,), jnp.float32, 0.0, math.log(3.0)))
    rough_cols = jnp.exp(jax.random.uniform(key_cols, (NY,), jnp.float32, 0.0, math.log(3.0)))
    scale = (ramp * rough_rows)[:, None, None] * rough_cols[None, :, None]
    noise = jnp.clip(jax.random.normal(key_noise, (3, NX, NY, NZ), jnp.float32), -6.0, 6.0)
    return jnp.clip(noise * scale, -64.0, 64.0)


def place_ends(drawn, key, low, high):
    dims = drawn.shape
    index_at = [jax.random.randint(jax.random.fold_in(key, axis), (), 0, dims[axis]) for axis in range(len(dims))]
    drawn = drawn.at[tuple(index_at)].set(low)
    longest = dims.index(max(dims))
    index_at[longest] = (index_at[longest] + 1) % dims[longest]
    return drawn.at[tuple(index_at)].set(high)


def setup_inputs(seed: int = 0) -> dict:
    splits = jax.random.split(jax.random.key(seed), 3)
    return {
        "right_side": draw_right_side(jax.random.fold_in(splits[2], 71), 0),
        "damage": place_ends(jax.random.randint(splits[1], (NX, NY, NZ), 0, 16), jax.random.fold_in(splits[1], 1), 0, 15).astype(jnp.int32),
    }


FLOOR_STIFFNESS = 0.05
MASS_TERM = 0.001
COUPLING = 2.5
RELAXATION = 0.6

def stiffness_of(damage):
    damage_level = damage.astype(jnp.float32) / 15.0
    return (1.0 - damage_level) ** 2 * (1.0 - FLOOR_STIFFNESS) + FLOOR_STIFFNESS

def diagonal_of(coefficient, mass_term):
    return coefficient * (6.0 + 2.0 * COUPLING) + mass_term

def stencil(padded, coefficient, mass_term):
    extent = (padded.shape[1] - 2, padded.shape[2] - 2, padded.shape[3] - 2)

    def neighbour(component, offset):
        return padded[component, 1 + offset[0]:1 + offset[0] + extent[0], 1 + offset[1]:1 + offset[1] + extent[1], 1 + offset[2]:1 + offset[2] + extent[2]]

    def joined(first, second, factor):
        return tuple((first[number] + factor * second[number] for number in range(3)))
    unit_steps = ((1, 0, 0), (0, 1, 0), (0, 0, 1))
    images = []
    for component in range(3):
        centre = neighbour(component, (0, 0, 0))
        beside_all = jnp.zeros_like(centre)
        for partner in range(3):
            step_up = unit_steps[partner]
            step_down = joined((0, 0, 0), step_up, -1)
            beside_all = beside_all + neighbour(component, step_up) + neighbour(component, step_down)
        own_up = unit_steps[component]
        own_down = joined((0, 0, 0), own_up, -1)
        axial_part = 2.0 * centre - neighbour(component, own_up) - neighbour(component, own_down)
        mixed_part = jnp.zeros_like(centre)
        for partner in range(3):
            if partner != component:
                other_up = unit_steps[partner]
                mixed_part = mixed_part + neighbour(partner, joined(own_up, other_up, 1)) - neighbour(partner, joined(own_up, other_up, -1)) - neighbour(partner, joined(own_down, other_up, 1)) + neighbour(partner, joined(own_down, other_up, -1))
        images.append(coefficient * (6.0 * centre - beside_all + COUPLING * (axial_part - 0.25 * mixed_part)) + mass_term * centre)
    return jnp.stack(images)

def apply_whole(displacement, coefficient):
    padded = jnp.pad(displacement, ((0, 0), (1, 1), (1, 1), (1, 1)))
    block_count = displacement.shape[1] // BLOCK

    def one_block(block_no):
        start = (block_no * BLOCK).astype(jnp.int32)
        slab_piece = lax.dynamic_slice_in_dim(padded, start, BLOCK + 2, 1)
        slab_stiff = lax.dynamic_slice_in_dim(coefficient, start, BLOCK, 0)
        return stencil(slab_piece, slab_stiff, MASS_TERM)
    blocks_out = lax.map(one_block, jnp.arange(block_count, dtype=jnp.int32))
    return jnp.moveaxis(blocks_out, 0, 1).reshape(displacement.shape)

def block_sums(source):
    channels, size_x, size_y, size_z = source.shape
    return lax.optimization_barrier(jnp.sum(source.reshape(channels, size_x // BLOCK, BLOCK, size_y // BLOCK, BLOCK, size_z // BLOCK, BLOCK), axis=(2, 4, 6)))

def spread(block_field):
    channels, size_x, size_y, size_z = block_field.shape
    widened = jnp.broadcast_to(block_field[:, :, None, :, None, :, None], (channels, size_x, BLOCK, size_y, BLOCK, size_z, BLOCK))
    return widened.reshape(channels, size_x * BLOCK, size_y * BLOCK, size_z * BLOCK)

def coarse_sweeps(coarse_load, mean_stiffness):
    coarse_coefficient = BLOCK ** 2 * mean_stiffness
    coarse_mass = BLOCK ** 3 * MASS_TERM
    coarse_diagonal = diagonal_of(coarse_coefficient, coarse_mass)
    correction = RELAXATION * coarse_load / coarse_diagonal
    for repeat in range(COARSE - 1):
        padded = jnp.pad(correction, ((0, 0), (1, 1), (1, 1), (1, 1)))
        coarse_image = stencil(padded, coarse_coefficient, coarse_mass)
        correction = correction + RELAXATION * (coarse_load - coarse_image) / coarse_diagonal
    return correction

def reference(right_side, damage):
    coefficient = stiffness_of(damage)
    diagonal = diagonal_of(coefficient, MASS_TERM)
    displacement = RELAXATION * right_side / diagonal
    displacement = displacement + RELAXATION * (right_side - apply_whole(displacement, coefficient)) / diagonal
    residual = right_side - apply_whole(displacement, coefficient)
    coarse_load = block_sums(residual)
    mean_stiffness = (block_sums(coefficient[None]) / BLOCK ** 3)[0]
    correction = coarse_sweeps(coarse_load, mean_stiffness)
    displacement = displacement + spread(correction)
    for repeat in range(2):
        displacement = displacement + RELAXATION * (right_side - apply_whole(displacement, coefficient)) / diagonal
    residual = right_side - apply_whole(displacement, coefficient)
    total_count = 3 * NX * NY * NZ
    load_sum = jnp.sum(right_side * right_side)
    residual_sum = jnp.sum(residual * residual)
    norms = jnp.stack([jnp.sqrt(load_sum / total_count), jnp.sqrt(residual_sum / total_count)])
    return (displacement, norms)
```

```python
import functools

import jax
import jax.numpy as jnp
from jax import lax
from jax.experimental import pallas as pl
from jax.experimental.pallas import tpu as pltpu
from jax.sharding import Mesh
from jax.sharding import PartitionSpec as P

BLOCK = 16
COARSE = 8
GX = ("gx_0", "gx_1")
GZ = ("gz_0", "gz_1")
ALL = ("gx_0", "gx_1", "gy", "gz_0", "gz_1")

FLOOR_STIFFNESS = 0.05
MASS_TERM = 0.001
COUPLING = 2.5
RELAXATION = 0.6

W = 4
NP = 16 + 2 * W
ROWS = 32
Y0 = 8
DIAG = 6.0 + 2.0 * COUPLING
OWN = 1.0 + COUPLING
MIX = 0.25 * COUPLING
KEEP = 1.0 - RELAXATION


def lanes_of(shape):
    return lax.broadcasted_iota(jnp.int32, shape, 1)


def rows_of(shape):
    return lax.broadcasted_iota(jnp.int32, shape, 0)


def stiffness_of(damage):
    level = damage.astype(jnp.float32) / 15.0
    return (1.0 - level) ** 2 * (1.0 - FLOOR_STIFFNESS) + FLOOR_STIFFNESS


def z_up(main, tail, lane):
    a = pltpu.roll(main, 127, 1)
    b = pltpu.roll(tail, 127, 1)
    last = lane == 127
    return jnp.where(last, b, a), jnp.where(last, a, b)


def z_down(main, tail, lane):
    a = pltpu.roll(main, 1, 1)
    b = pltpu.roll(tail, 1, 1)
    first = lane == 0
    return jnp.where(first, b, a), jnp.where(first, a, b)


def neighbour_sum(ref, i, row, lane, both):
    def at(c, dx, dy, t):
        return ref[c, i + dx, t, pl.ds(row + dy, 8), :]

    ups, downs, rests, centres = [], [], [], []
    for t in range(2):
        v = [at(c, 0, 0, t) for c in range(3)]
        xp = [at(c, 1, 0, t) for c in range(3)]
        xm = [at(c, -1, 0, t) for c in range(3)]
        yp = [at(c, 0, 1, t) for c in range(3)]
        ym = [at(c, 0, -1, t) for c in range(3)]
        zx = MIX * (xp[2] - xm[2])
        zy = MIX * (yp[2] - ym[2])
        zz = MIX * ((xp[0] - xm[0]) + (yp[1] - ym[1]))
        own = OWN * v[2]
        ups.append((v[0] + zx, v[1] + zy, own + zz))
        downs.append((v[0] - zx, v[1] - zy, own - zz))
        centres.append(v)
        if t == 0 or both:
            mix_x = (at(1, 1, 1, t) - at(1, 1, -1, t)) - (at(1, -1, 1, t) - at(1, -1, -1, t))
            mix_y = (at(0, 1, 1, t) - at(0, 1, -1, t)) - (at(0, -1, 1, t) - at(0, -1, -1, t))
            rests.append(
                (
                    OWN * (xp[0] + xm[0]) + (yp[0] + ym[0]) + MIX * mix_x,
                    OWN * (yp[1] + ym[1]) + (xp[1] + xm[1]) + MIX * mix_y,
                    (xp[2] + xm[2]) + (yp[2] + ym[2]),
                )
            )
    sums = [[], []]
    for c in range(3):
        up = z_up(ups[0][c], ups[1][c], lane)
        down = z_down(downs[0][c], downs[1][c], lane)
        for t in range(2 if both else 1):
            sums[t].append(rests[t][c] + (up[t] + down[t]))
    return sums, centres


def sweep(source, target, p_ref, q_ref, first, last):
    lane = lanes_of((8, 128))

    def plane(i, carry):
        for row in (4, 12, 20):
            sums, centres = neighbour_sum(source, i, row, lane, True)
            for t in range(2):
                q = q_ref[i, t, pl.ds(row, 8), :]
                for c in range(3):
                    p = p_ref[c, i, t, pl.ds(row, 8), :]
                    target[c, i, t, pl.ds(row, 8), :] = KEEP * centres[t][c] + p + q * sums[t][c]
        return carry

    lax.fori_loop(first, last, plane, 0)


def first_kernel(at_ref, wide, zlo, zhi, x2, p_ref, q_ref, sums_out):
    lane24 = lanes_of((NP, 128))
    row24 = rows_of((NP, 128))
    lane = lanes_of((8, 128))
    gx, gy, gz = at_ref[0], at_ref[1], at_ref[2]
    y = gy * 16 + row24 - W
    y_in = (y >= 0) & (y < at_ref[4])
    tail_in = ((lane24 < W) & (gz < at_ref[5] - 1)) | ((lane24 >= 128 - W) & (gz > 0))

    def prepare(i, carry):
        x = gx * 16 + i - W
        x_in = (x >= 0) & (x < at_ref[3])
        for t in range(2):
            if t == 0:
                parts = [wide[c, i] for c in range(4)]
                inside = y_in & x_in
            else:
                parts = [
                    jnp.where(
                        lane24 < W,
                        pltpu.roll(zhi[c], (128 - W * i) % 128, 1),
                        pltpu.roll(zlo[c], 128 - W - W * i, 1),
                    )
                    for c in range(4)
                ]
                inside = y_in & x_in & tail_in
            g = stiffness_of(parts[3])
            scale = RELAXATION / (g * DIAG + MASS_TERM)
            for c in range(3):
                value = parts[c] * scale
                if t == 1:
                    value = jnp.where(tail_in, value, 0.0)
                p_ref[c, i, t, pl.ds(4, NP), :] = value
            q_ref[i, t, pl.ds(4, NP), :] = jnp.where(inside, g * scale, 0.0)
        return carry

    lax.fori_loop(0, NP, prepare, 0)
    sweep(p_ref, x2, p_ref, q_ref, 1, NP - 1)

    def residual(i, carry):
        totals = list(carry)
        for row in (8, 16):
            sums, centres = neighbour_sum(x2, i, row, lane, False)
            g = stiffness_of(wide[3, i, pl.ds(row - 4, 8), :])
            d = g * DIAG + MASS_TERM
            for c in range(3):
                f = wide[c, i, pl.ds(row - 4, 8), :]
                totals[c] += (f - d * centres[0][c]) + g * sums[0][c]
                totals[4] += f * f
            totals[3] += g
        return tuple(totals)

    zero = jnp.zeros((8, 128), jnp.float32)
    totals = lax.fori_loop(W, W + 16, residual, (zero,) * 5)
    row = rows_of((8, 128))
    stacked = zero
    for c in range(5):
        stacked = jnp.where(row == c, jnp.sum(totals[c], axis=0, keepdims=True), stacked)
    big = (128, 128)
    gather = (rows_of(big) // BLOCK == lanes_of(big) % 8).astype(jnp.float32)
    by_cell = jnp.dot(
        stacked, gather, precision=lax.Precision.HIGHEST, preferred_element_type=jnp.float32
    )
    slot = jnp.sum(jnp.where(lane // 8 == row, by_cell, 0.0), axis=0, keepdims=True)
    sums_out[...] = jnp.broadcast_to(slot, sums_out.shape)


def coarse_solve(load, mean, gx_n, gy_n, gz_n):
    shape = load[0].shape
    n = shape[1]
    lane = lanes_of(shape)
    row = rows_of(shape)
    sx, sy = gy_n * gz_n, gz_n
    x_at, y_at, z_at = lane // sx, lane // sy % gy_n, lane % gz_n

    def shift(v, step, at, count):
        up = jnp.where(at < count - 1, pltpu.roll(v, n - step, 1), 0.0)
        down = jnp.where(at > 0, pltpu.roll(v, step, 1), 0.0)
        return up, down

    def shift_z(v):
        up = pltpu.roll(v, 7, 0)
        down = pltpu.roll(v, 1, 0)
        next_up = jnp.where(z_at < gz_n - 1, pltpu.roll(up, n - 1, 1), 0.0)
        next_down = jnp.where(z_at > 0, pltpu.roll(down, 1, 1), 0.0)
        return jnp.where(row == 7, next_up, up), jnp.where(row == 0, next_down, down)

    shifts = (
        lambda v: shift(v, sx, x_at, gx_n),
        lambda v: shift(v, sy, y_at, gy_n),
        shift_z,
    )
    coefficient = BLOCK**2 * mean
    scale = RELAXATION / (coefficient * DIAG + BLOCK**3 * MASS_TERM)
    p = [scale * value for value in load]
    q = scale * coefficient

    def step(_, w):
        pairs = [[shifts[b](w[a]) for b in range(3)] for a in range(3)]
        diffs = [pairs[a][a][0] - pairs[a][a][1] for a in range(3)]
        out = []
        for a in range(3):
            total = 0.0
            for b in range(3):
                both = pairs[a][b][0] + pairs[a][b][1]
                total = total + (OWN * both if a == b else both)
            others = [diffs[b] for b in range(3) if b != a]
            up, down = shifts[a](others[0] + others[1])
            out.append(KEEP * w[a] + p[a] + q * (total + MIX * (up - down)))
        return tuple(out)

    return lax.fori_loop(0, COARSE - 1, step, tuple(p))


def second_kernel(
    counts, at_ref, every, x2, p_ref, q_ref, damage, out, sum_out, load_out, x3, x4, w_ref
):
    gx_n, gy_n, gz_n = counts
    lane = lanes_of((8, 128))
    row8 = rows_of((8, 128))
    cells = jnp.transpose(every[...])
    load = [cells[8 * c : 8 * c + 8] for c in range(3)]
    mean = cells[24:32] * (1.0 / BLOCK**3)
    load_out[...] = jnp.broadcast_to(jnp.sum(cells[32:40]), load_out.shape)
    w = coarse_solve(load, mean, gx_n, gy_n, gz_n)
    n = gx_n * gy_n * gz_n
    me = at_ref[6]
    centre = n // 2
    pick = (lane // BLOCK == row8).astype(jnp.float32)
    for c in range(3):
        turned = pltpu.roll(w[c], (centre + n - me) % n, 1)
        for dx in range(3):
            for dy in range(3):
                j = centre + (dx - 1) * gy_n * gz_n + (dy - 1) * gz_n
                main = jnp.sum(turned[:, j : j + 1] * pick, axis=0, keepdims=True)
                high = jnp.broadcast_to(turned[0:1, j + 1 : j + 2], (1, 128))
                low = jnp.broadcast_to(turned[7:8, j - 1 : j], (1, 128))
                tail = jnp.where(lane[:1] < W, high, low)
                first, size = ((4, 4), (8, 16), (24, 4))[dy]
                w_ref[c, dx, 0, pl.ds(first, size), :] = jnp.broadcast_to(main, (size, 128))
                w_ref[c, dx, 1, pl.ds(first, size), :] = jnp.broadcast_to(tail, (size, 128))

    def correct(i, carry):
        cell = (i >= W).astype(jnp.int32) + (i >= W + 16).astype(jnp.int32)
        for t in range(2):
            inside = q_ref[i, t, pl.ds(4, NP), :] > 0.0
            for c in range(3):
                value = w_ref[c, cell, t, pl.ds(4, NP), :]
                x3[c, i, t, pl.ds(4, NP), :] = x2[c, i, t, pl.ds(4, NP), :] + jnp.where(
                    inside, value, 0.0
                )
        return carry

    lax.fori_loop(1, NP - 1, correct, 0)
    sweep(x3, x4, p_ref, q_ref, 2, NP - 2)
    sweep(x4, x3, p_ref, q_ref, 3, NP - 3)

    def residual(i, total):
        for row in (8, 16):
            sums, centres = neighbour_sum(x3, i, row, lane, False)
            g = stiffness_of(damage[i - W, pl.ds(row - 8, 8), :])
            d = (g * DIAG + MASS_TERM) * (1.0 / RELAXATION)
            q = q_ref[i, 0, pl.ds(row, 8), :]
            for c in range(3):
                p = p_ref[c, i, 0, pl.ds(row, 8), :]
                out[c, i - W, pl.ds(row - 8, 8), :] = centres[0][c]
                r = d * ((p - RELAXATION * centres[0][c]) + q * sums[0][c])
                total += r * r
        return total

    total = lax.fori_loop(W, W + 16, residual, jnp.zeros((8, 128), jnp.float32))
    sum_out[...] = jnp.broadcast_to(jnp.sum(total), sum_out.shape)


def pack_kernel(wide, low_out, high_out):
    lane = lanes_of((NP, 128))
    for c in range(4):
        low = jnp.zeros((NP, 128), jnp.float32)
        high = low
        for i in range(NP):
            value = wide[c, i]
            here = (lane >= W * i) & (lane < W * i + W)
            low = jnp.where(here, pltpu.roll(value, W * i, 1), low)
            high = jnp.where(here, pltpu.roll(value, (W * i + W) % 128, 1), high)
        low_out[c] = low
        high_out[c] = high


def beside(block, axis, dim):
    count = lax.axis_size(axis)
    forward = [(i, i + 1) for i in range(count - 1)]
    backward = [(i + 1, i) for i in range(count - 1)]
    low = lax.ppermute(
        lax.slice_in_dim(block, block.shape[dim] - W, None, axis=dim), axis, forward
    )
    high = lax.ppermute(lax.slice_in_dim(block, 0, W, axis=dim), axis, backward)
    return jnp.concatenate([low, block, high], axis=dim)


VMEM = pl.BlockSpec(memory_space=pltpu.VMEM)
SMEM = pl.BlockSpec(memory_space=pltpu.SMEM)
F32 = jnp.float32


def on_device(right_side, damage):
    gx_n, gy_n, gz_n = lax.axis_size(GX), lax.axis_size("gy"), lax.axis_size(GZ)
    n = gx_n * gy_n * gz_n
    gx, gy, gz = lax.axis_index(GX), lax.axis_index("gy"), lax.axis_index(GZ)
    at = jnp.stack(
        [
            gx,
            gy,
            gz,
            jnp.int32(gx_n * 16),
            jnp.int32(gy_n * 16),
            jnp.int32(gz_n),
            (gx * gy_n + gy) * gz_n + gz,
        ]
    ).astype(jnp.int32)
    stacked = jnp.concatenate([right_side, damage.astype(F32)[None]], axis=0)
    wide = beside(beside(stacked, GX, 1), "gy", 2)
    side = jax.ShapeDtypeStruct((4, NP, 128), F32)
    low, high = pl.pallas_call(
        pack_kernel, out_shape=(side, side), in_specs=[VMEM], out_specs=(VMEM, VMEM)
    )(wide)
    zlo = lax.ppermute(high, GZ, [(i, i + 1) for i in range(gz_n - 1)])
    zhi = lax.ppermute(low, GZ, [(i + 1, i) for i in range(gz_n - 1)])
    field = (3, NP, 2, ROWS, 128)
    x2, p, q, sums = pl.pallas_call(
        first_kernel,
        out_shape=(
            jax.ShapeDtypeStruct(field, F32),
            jax.ShapeDtypeStruct(field, F32),
            jax.ShapeDtypeStruct(field[1:], F32),
            jax.ShapeDtypeStruct((n, 128), F32),
        ),
        in_specs=[SMEM, VMEM, VMEM, VMEM],
        out_specs=(VMEM,) * 4,
    )(at, wide, zlo, zhi)
    every = lax.all_to_all(sums, ALL, 0, 0, tiled=True)
    displacement, residual_sums, load_sum = pl.pallas_call(
        functools.partial(second_kernel, (gx_n, gy_n, gz_n)),
        out_shape=(
            jax.ShapeDtypeStruct(right_side.shape, F32),
            jax.ShapeDtypeStruct((n, 128), F32),
            jax.ShapeDtypeStruct((1, 128), F32),
        ),
        in_specs=[SMEM] + [VMEM] * 5,
        out_specs=(VMEM,) * 3,
        scratch_shapes=[
            pltpu.VMEM(field, F32),
            pltpu.VMEM(field, F32),
            pltpu.VMEM((3, 3, 2, ROWS, 128), F32),
        ],
    )(at, every, x2, p, q, damage)
    residual_sum = jnp.sum(lax.all_to_all(residual_sums[:, :1], ALL, 0, 0, tiled=True))
    total_count = right_side.size * n
    norms = jnp.sqrt(jnp.stack([load_sum[0, 0], residual_sum]) / total_count)
    return (displacement, norms)


def solution(mesh):
    torus = Mesh(mesh.devices.reshape(4, 2, mesh.shape["gy"], 2, 4), ALL)
    placed = (P(None, GX, "gy", GZ), P(GX, "gy", GZ))
    return jax.shard_map(
        on_device,
        mesh=torus,
        in_specs=placed,
        out_specs=(P(None, GX, "gy", GZ), P()),
        check_vma=False,
    )
```

```python
import functools

import jax
import jax.numpy as jnp
from jax import lax
from jax.experimental import pallas as pl
from jax.experimental.pallas import tpu as pltpu
from jax.sharding import Mesh
from jax.sharding import PartitionSpec as P

BLOCK = 16
COARSE = 8
GX = ("gx_0", "gx_1")
GZ = ("gz_0", "gz_1")
ALL = ("gx_0", "gx_1", "gy", "gz_0", "gz_1")

FLOOR_STIFFNESS = 0.05
MASS_TERM = 0.001
COUPLING = 2.5
RELAXATION = 0.6

W = 4
NP = 16 + 2 * W
ROWS = 40
GROUPS = (4, 12, 20)
OWN_GROUPS = (8, 16)
DIAG = 6.0 + 2.0 * COUPLING
OWN = 1.0 + COUPLING
MIX = 0.25 * COUPLING
KEEP = 1.0 - RELAXATION
F32 = jnp.float32


def lanes_of(shape):
    return lax.broadcasted_iota(jnp.int32, shape, 1)


def rows_of(shape):
    return lax.broadcasted_iota(jnp.int32, shape, 0)


def stiffness_of(damage):
    level = damage.astype(F32) / 15.0
    return (1.0 - level) ** 2 * (1.0 - FLOOR_STIFFNESS) + FLOOR_STIFFNESS


def position(axis):
    at = lax.axis_index(axis)
    return at, lax.axis_size(axis), at % 2


def pick(odd, when_odd, when_even):
    return jnp.where(odd, when_odd, when_even)


def tail_edges(tail, row, page, up):
    parts = tail_parts(tail, row, page)
    return parts[0] if up else parts[1]


def tail_parts(tail, row, page):
    v = [tail[page, c, pl.ds(row, 8), :] for c in range(3)]
    yp = [tail[page, c, pl.ds(row + 1, 8), :] for c in range(3)]
    ym = [tail[page, c, pl.ds(row - 1, 8), :] for c in range(3)]
    xp = [pltpu.roll(v[c], 128 - W, 1) for c in range(3)]
    xm = [pltpu.roll(v[c], W, 1) for c in range(3)]
    zx = MIX * (xp[2] - xm[2])
    zy = MIX * (yp[2] - ym[2])
    zz = MIX * ((xp[0] - xm[0]) + (yp[1] - ym[1]))
    own = OWN * v[2]
    ups = (v[0] + zx, v[1] + zy, own + zz)
    downs = (v[0] - zx, v[1] - zy, own - zz)
    return ups, downs, v, xp, xm, yp, ym


def tail_sweep(source, target, pq, edges, outer_only=False):
    lane = lanes_of((8, 128))
    first = lane % W == 0
    last = lane % W == W - 1
    for row in GROUPS:
        for low in (0, 2):
            parts = [tail_parts(source, row, page) for page in (low, low + 1)]
            (up_a, down_a), (up_b, down_b) = (part[:2] for part in parts)
            for c in range(3):
                if low == 0:
                    edges[3 + c, pl.ds(row, 8), :] = down_a[c]
                else:
                    edges[c, pl.ds(row, 8), :] = up_b[c]
            sums = (
                [
                    jnp.where(last, pltpu.roll(up_b[c], W - 1, 1), pltpu.roll(up_a[c], 127, 1))
                    + pltpu.roll(down_a[c], 1, 1)
                    for c in range(3)
                ],
                [
                    jnp.where(first, pltpu.roll(down_a[c], 129 - W, 1), pltpu.roll(down_b[c], 1, 1))
                    + pltpu.roll(up_b[c], 127, 1)
                    for c in range(3)
                ],
            )
            for t in range(2):
                if outer_only and low + t in (1, 2):
                    continue
                _, _, v, xp, xm, yp, ym = parts[t]
                dy0 = MIX * (yp[0] - ym[0])
                dy1 = MIX * (yp[1] - ym[1])
                mix_x = pltpu.roll(dy1, 128 - W, 1) - pltpu.roll(dy1, W, 1)
                mix_y = pltpu.roll(dy0, 128 - W, 1) - pltpu.roll(dy0, W, 1)
                rest = (
                    OWN * (xp[0] + xm[0]) + (yp[0] + ym[0]) + mix_x,
                    OWN * (yp[1] + ym[1]) + (xp[1] + xm[1]) + mix_y,
                    (xp[2] + xm[2]) + (yp[2] + ym[2]),
                )
                q = pq[low + t, 3, pl.ds(row, 8), :]
                for c in range(3):
                    p = pq[low + t, c, pl.ds(row, 8), :]
                    target[low + t, c, pl.ds(row, 8), :] = (
                        KEEP * v[c] + p + q * (rest[c] + sums[t][c])
                    )


def edges_only(source, edges):
    for row in OWN_GROUPS:
        ups = tail_parts(source, row, 3)[0]
        downs = tail_parts(source, row, 0)[1]
        for c in range(3):
            edges[c, pl.ds(row, 8), :] = ups[c]
            edges[3 + c, pl.ds(row, 8), :] = downs[c]


def neighbour_sum(ref, edges, i, row, lane):
    def at(c, dx, dy):
        return ref[i + dx, c, pl.ds(row + dy, 8), :]

    v = [at(c, 0, 0) for c in range(3)]
    xp = [at(c, 1, 0) for c in range(3)]
    xm = [at(c, -1, 0) for c in range(3)]
    yp = [at(c, 0, 1) for c in range(3)]
    ym = [at(c, 0, -1) for c in range(3)]
    zx = MIX * (xp[2] - xm[2])
    zy = MIX * (yp[2] - ym[2])
    zz = MIX * ((xp[0] - xm[0]) + (yp[1] - ym[1]))
    own = OWN * v[2]
    ups = (v[0] + zx, v[1] + zy, own + zz)
    downs = (v[0] - zx, v[1] - zy, own - zz)
    mix_x = (at(1, 1, 1) - at(1, 1, -1)) - (at(1, -1, 1) - at(1, -1, -1))
    mix_y = (at(0, 1, 1) - at(0, 1, -1)) - (at(0, -1, 1) - at(0, -1, -1))
    rest = (
        OWN * (xp[0] + xm[0]) + (yp[0] + ym[0]) + MIX * mix_x,
        OWN * (yp[1] + ym[1]) + (xp[1] + xm[1]) + MIX * mix_y,
        (xp[2] + xm[2]) + (yp[2] + ym[2]),
    )
    sums = []
    for c in range(3):
        high = pltpu.roll(edges[c, pl.ds(row, 8), :], 127 - W * i, 1)
        low = pltpu.roll(edges[3 + c, pl.ds(row, 8), :], 129 - W - W * i, 1)
        up = jnp.where(lane == 127, high, pltpu.roll(ups[c], 127, 1))
        down = jnp.where(lane == 0, low, pltpu.roll(downs[c], 1, 1))
        sums.append(rest[c] + (up + down))
    return sums, v


def sweep(source, target, pq, edges, first, last):
    lane = lanes_of((8, 128))

    def plane(i, carry):
        for row in GROUPS:
            sums, v = neighbour_sum(source, edges, i, row, lane)
            q = pq[i, 3, pl.ds(row, 8), :]
            for c in range(3):
                p = pq[i, c, pl.ds(row, 8), :]
                target[i, c, pl.ds(row, 8), :] = KEEP * v[c] + p + q * sums[c]
        return carry

    lax.fori_loop(first, last, plane, 0, unroll=2)


def x_pack_kernel(load, damage, f_out, far_out, near_out, level, load_sem, level_sem):
    odd = position(GX)[2] == 1
    load_copy = pltpu.make_async_copy(load, f_out.at[pl.ds(0, 3)], load_sem)
    level_copy = pltpu.make_async_copy(damage, level, level_sem)
    load_copy.start()
    level_copy.start()
    level_copy.wait()
    f_out[3] = level[...].astype(F32)
    load_copy.wait()
    for c in range(4):
        for i in range(W):
            low, high = f_out[c, i], f_out[c, i + 16 - W]
            far_out[c, i] = pick(odd, high, low)
            near_out[c, i] = pick(odd, low, high)


def y_pack_kernel(f, xfar, xnear, far_out, near_out):
    odd_x, odd_y = position(GX)[2] == 1, position("gy")[2] == 1
    upper = rows_of((8, 128)) < 4

    def tile(c, i, k):
        rows = pl.ds(8 * k, 8)
        if i < W:
            return pick(odd_x, xnear[c, i, rows, :], xfar[c, i, rows, :])
        if i >= W + 16:
            return pick(odd_x, xfar[c, i - W - 16, rows, :], xnear[c, i - W - 16, rows, :])
        return f[c, i - W, rows, :]

    for c in range(4):
        for j in range(NP // 2):
            a, b = 2 * j, 2 * j + 1
            low = jnp.where(upper, tile(c, a, 0), pltpu.roll(tile(c, b, 0), 4, 0))
            high = jnp.where(upper, pltpu.roll(tile(c, a, 1), 4, 0), tile(c, b, 1))
            far_out[c, j] = pick(odd_y, high, low)
            near_out[c, j] = pick(odd_y, low, high)


def z_pack_kernel(f, xfar, xnear, yfar, ynear, far_out, near_out):
    odd_x, odd_y, odd_z = position(GX)[2] == 1, position("gy")[2] == 1, position(GZ)[2]
    lane = lanes_of((8, 128))
    upper = rows_of((8, 128)) < 4
    for c in range(4):
        for k in range(3):
            far = jnp.zeros((8, 128), F32)
            near = far
            for i in range(NP):
                if k == 2:
                    low = pick(odd_y, ynear[c, i // 2], yfar[c, i // 2])
                    high = pick(odd_y, yfar[c, i // 2], ynear[c, i // 2])
                    if i % 2:
                        value = jnp.where(upper, pltpu.roll(low, 4, 0), high)
                    else:
                        value = jnp.where(upper, low, pltpu.roll(high, 4, 0))
                else:
                    rows = pl.ds(8 * k, 8)
                    if i < W:
                        value = pick(odd_x, xnear[c, i, rows, :], xfar[c, i, rows, :])
                    elif i >= W + 16:
                        j = i - W - 16
                        value = pick(odd_x, xfar[c, j, rows, :], xnear[c, j, rows, :])
                    else:
                        value = f[c, i - W, rows, :]
                here = (lane >= W * i) & (lane < W * i + W)
                far = jnp.where(here, pltpu.roll(value, W * i + W * odd_z, 1), far)
                near = jnp.where(here, pltpu.roll(value, W * i + W * (1 - odd_z), 1), near)
            far_out[c, pl.ds(8 * k, 8), :] = far
            near_out[c, pl.ds(8 * k, 8), :] = near


def main_kernel(f, xfar, xnear, yfar, ynear, pq):
    gx, gx_n, odd_x = position(GX)
    gy, gy_n, odd_y = position("gy")
    odd_x, odd_y = odd_x == 1, odd_y == 1

    def x_inside(i):
        x = gx * 16 + i - W
        return (x >= 0) & (x < gx_n * 16)

    def values(parts, inside):
        g = stiffness_of(parts[3])
        scale = RELAXATION / (g * DIAG + MASS_TERM)
        out = [part * scale for part in parts[:3]] + [g * scale]
        return [jnp.where(inside, value, 0.0) for value in out]

    def fill(i, parts):
        for c, value in enumerate(values(parts, x_inside(i))):
            pq[i, c, pl.ds(8, 16), :] = value

    def own(i, carry):
        fill(i, [f[c, i - W] for c in range(4)])
        return carry

    lax.fori_loop(W, W + 16, own, 0)

    def beside_x(i, carry):
        fill(i, [pick(odd_x, xnear[c, i], xfar[c, i]) for c in range(4)])
        fill(i + W + 16, [pick(odd_x, xfar[c, i], xnear[c, i]) for c in range(4)])
        return carry

    lax.fori_loop(0, W, beside_x, 0)
    second = (rows_of((8, 128)) >= 4).astype(jnp.int32)
    low_in, high_in = gy > 0, gy < gy_n - 1

    def beside_y(j, carry):
        inside = x_inside(2 * j + second)
        low = values([pick(odd_y, ynear[c, j], yfar[c, j]) for c in range(4)], inside & low_in)
        high = values([pick(odd_y, yfar[c, j], ynear[c, j]) for c in range(4)], inside & high_in)
        for c in range(4):
            for t in range(2):
                pq[2 * j + t, c, pl.ds(4, 4), :] = low[c][4 * t : 4 * t + 4]
                pq[2 * j + t, c, pl.ds(24, 4), :] = high[c][4 * t : 4 * t + 4]
        return carry

    lax.fori_loop(0, NP // 2, beside_y, 0)


def first_kernel(
    pq, f, zfar_own, znear_own, zfar, znear, x2, tail, tail_pq, sums_out, edges
):
    lane = lanes_of((8, 128))
    row8 = rows_of((8, 128))
    gx, gx_n, _ = position(GX)
    gy, gy_n, _ = position("gy")
    gz, gz_n, odd_z = position(GZ)
    odd_z = odd_z == 1
    x = gx * 16 + lane // W - W
    x_in = (x >= 0) & (x < gx_n * 16)
    y_in = ((row8 >= 4) | (gy > 0)) & ((row8 < 4) | (gy < gy_n - 1))
    z_in = (gz > 0, True, True, gz < gz_n - 1)
    sides = (
        (znear, zfar),
        (znear_own, zfar_own),
        (zfar_own, znear_own),
        (zfar, znear),
    )
    for page in range(4):
        when_odd, when_even = sides[page]
        for k in range(3):
            rows = pl.ds(8 * k, 8)
            parts = [pick(odd_z, when_odd[c, rows, :], when_even[c, rows, :]) for c in range(4)]
            g = stiffness_of(parts[3])
            scale = RELAXATION / (g * DIAG + MASS_TERM)
            inside = x_in
            if page in (0, 3):
                inside = inside & z_in[page]
            if k == 2:
                inside = inside & y_in
            for c in range(4):
                value = jnp.where(inside, (parts[c] if c < 3 else g) * scale, 0.0)
                if k < 2:
                    tail_pq[page, c, pl.ds(8 + 8 * k, 8), :] = value
                else:
                    tail_pq[page, c, pl.ds(4, 4), :] = value[:4]
                    tail_pq[page, c, pl.ds(24, 4), :] = value[4:]
    tail_sweep(tail_pq, tail, tail_pq, edges)
    sweep(pq, x2, pq, edges, 1, NP - 1)
    edges_only(tail, edges)

    def residual(i, carry):
        totals = list(carry)
        for row in OWN_GROUPS:
            sums, v = neighbour_sum(x2, edges, i, row, lane)
            rows = pl.ds(row - 8, 8)
            g = stiffness_of(f[3, i - W, rows, :])
            d = g * DIAG + MASS_TERM
            for c in range(3):
                load = f[c, i - W, rows, :]
                totals[c] += (load - d * v[c]) + g * sums[c]
                totals[4] += load * load
            totals[3] += g
        return tuple(totals)

    zero = jnp.zeros((8, 128), F32)
    totals = lax.fori_loop(W, W + 16, residual, (zero,) * 5, unroll=2)
    stacked = zero
    for c in range(5):
        stacked = jnp.where(row8 == c, jnp.sum(totals[c], axis=0, keepdims=True), stacked)
    big = (128, 128)
    gather = (rows_of(big) // BLOCK == lanes_of(big) % 8).astype(F32)
    by_cell = jnp.dot(
        stacked, gather, precision=lax.Precision.HIGHEST, preferred_element_type=F32
    )
    slot = jnp.sum(jnp.where(lane // 8 == row8, by_cell, 0.0), axis=0, keepdims=True)
    sums_out[...] = jnp.broadcast_to(slot, sums_out.shape)


def coarse_solve(load, mean, gx_n, gy_n, gz_n):
    shape = load[0].shape
    n = shape[1]
    lane = lanes_of(shape)
    row = rows_of(shape)
    sx, sy = gy_n * gz_n, gz_n
    x_at, y_at, z_at = lane // sx, lane // sy % gy_n, lane % gz_n

    def shift(v, step, at, count):
        up = jnp.where(at < count - 1, pltpu.roll(v, n - step, 1), 0.0)
        down = jnp.where(at > 0, pltpu.roll(v, step, 1), 0.0)
        return up, down

    def shift_z(v):
        up = pltpu.roll(v, 7, 0)
        down = pltpu.roll(v, 1, 0)
        next_up = jnp.where(z_at < gz_n - 1, pltpu.roll(up, n - 1, 1), 0.0)
        next_down = jnp.where(z_at > 0, pltpu.roll(down, 1, 1), 0.0)
        return jnp.where(row == 7, next_up, up), jnp.where(row == 0, next_down, down)

    shifts = (
        lambda v: shift(v, sx, x_at, gx_n),
        lambda v: shift(v, sy, y_at, gy_n),
        shift_z,
    )
    coefficient = BLOCK**2 * mean
    scale = RELAXATION / (coefficient * DIAG + BLOCK**3 * MASS_TERM)
    p = [scale * value for value in load]
    q = scale * coefficient

    def step(_, w):
        pairs = [[shifts[b](w[a]) for b in range(3)] for a in range(3)]
        diffs = [pairs[a][a][0] - pairs[a][a][1] for a in range(3)]
        out = []
        for a in range(3):
            total = 0.0
            for b in range(3):
                both = pairs[a][b][0] + pairs[a][b][1]
                total = total + (OWN * both if a == b else both)
            others = [diffs[b] for b in range(3) if b != a]
            up, down = shifts[a](others[0] + others[1])
            out.append(KEEP * w[a] + p[a] + q * (total + MIX * (up - down)))
        return tuple(out)

    return lax.fori_loop(0, COARSE - 1, step, tuple(p))


def second_kernel(
    every,
    x2,
    tail2,
    pq,
    tail_pq,
    f,
    out,
    sum_out,
    x3,
    x4,
    tail3,
    tail4,
    w_ref,
    edges,
    out_sem,
):
    gx, gx_n, _ = position(GX)
    gy, gy_n, _ = position("gy")
    gz, gz_n, _ = position(GZ)
    me = (gx * gy_n + gy) * gz_n + gz
    lane = lanes_of((8, 128))
    row8 = rows_of((8, 128))
    cells = jnp.transpose(every[...])
    load = [cells[8 * c : 8 * c + 8] for c in range(3)]
    mean = cells[24:32] * (1.0 / BLOCK**3)
    load_sum = jnp.sum(cells[32:40])
    w = coarse_solve(load, mean, gx_n, gy_n, gz_n)
    n = gx_n * gy_n * gz_n
    centre = n // 2
    own_cells = (lane // BLOCK == row8).astype(F32)
    line = lane[:1]
    cell_of = ((7, -1), (0, 0), (7, 0), (0, 1))
    spans = ((4, 4), (8, 16), (24, 4))
    for c in range(3):
        turned = pltpu.roll(w[c], (centre + n - me) % n, 1)

        def column(dx, dy):
            return centre + (dx - 1) * gy_n * gz_n + (dy - 1) * gz_n

        for dy in range(3):
            first, size = spans[dy]
            for dx in range(3):
                j = column(dx, dy)
                main = jnp.sum(turned[:, j : j + 1] * own_cells, axis=0, keepdims=True)
                w_ref[dx, c, pl.ds(first, size), :] = jnp.broadcast_to(main, (size, 128))
            for page in range(4):
                k, dz = cell_of[page]
                here = [
                    jnp.broadcast_to(
                        turned[k : k + 1, column(dx, dy) + dz : column(dx, dy) + dz + 1], (1, 128)
                    )
                    for dx in range(3)
                ]
                value = jnp.where(
                    line < W * W, here[0], jnp.where(line < W * (W + 16), here[1], here[2])
                )
                rows = pl.ds(first, size)
                inside = tail_pq[page, 3, rows, :] > 0.0
                tail3[page, c, rows, :] = tail2[page, c, rows, :] + jnp.where(inside, value, 0.0)

    def correct(i, carry):
        cell = (i >= W).astype(jnp.int32) + (i >= W + 16).astype(jnp.int32)
        for row in GROUPS:
            rows = pl.ds(row, 8)
            inside = pq[i, 3, rows, :] > 0.0
            for c in range(3):
                x3[i, c, rows, :] = x2[i, c, rows, :] + jnp.where(
                    inside, w_ref[cell, c, rows, :], 0.0
                )
        return carry

    lax.fori_loop(1, NP - 1, correct, 0)
    tail_sweep(tail3, tail4, tail_pq, edges)
    sweep(x3, x4, pq, edges, 2, NP - 2)
    tail_sweep(tail4, tail3, tail_pq, edges, True)
    sweep(x4, x3, pq, edges, 3, NP - 3)
    copies = [
        pltpu.make_async_copy(
            x3.at[pl.ds(W, 16), c, pl.ds(8, 16), :], out.at[c], out_sem.at[c]
        )
        for c in range(3)
    ]
    for copy in copies:
        copy.start()
    edges_only(tail3, edges)

    def residual(i, total):
        for row in OWN_GROUPS:
            sums, v = neighbour_sum(x3, edges, i, row, lane)
            rows = pl.ds(row - 8, 8)
            g = stiffness_of(f[3, i - W, rows, :])
            d = (g * DIAG + MASS_TERM) * (1.0 / RELAXATION)
            q = pq[i, 3, pl.ds(row, 8), :]
            for c in range(3):
                p = pq[i, c, pl.ds(row, 8), :]
                r = d * ((p - RELAXATION * v[c]) + q * sums[c])
                total += r * r
        return total

    total = jnp.sum(lax.fori_loop(W, W + 16, residual, jnp.zeros((8, 128), F32), unroll=2))
    both = jnp.where(line == 0, load_sum * (1.0 / n), total)
    sum_out[...] = jnp.broadcast_to(both, sum_out.shape)
    for copy in copies:
        copy.wait()


def swaps(far_send, near_send, axis):
    count = lax.axis_size(axis)
    near = [(i, i ^ 1) for i in range(count)]
    far = [(i, ((i ^ 1) + (2 if i % 2 else -2)) % count) for i in range(count)]
    return lax.ppermute(far_send, axis, far), lax.ppermute(near_send, axis, near)


VMEM = pl.BlockSpec(memory_space=pltpu.VMEM)
SMEM = pl.BlockSpec(memory_space=pltpu.SMEM)
HBM = pl.BlockSpec(memory_space=pltpu.HBM)


def call(kernel, shapes, arguments, mib, scratch=(), source=VMEM, target=VMEM):
    shapes = [jax.ShapeDtypeStruct(shape, F32) for shape in shapes]
    return pl.pallas_call(
        kernel,
        out_shape=tuple(shapes),
        in_specs=[source] * len(arguments),
        out_specs=target if isinstance(target, tuple) else (target,) * len(shapes),
        scratch_shapes=[pltpu.VMEM(s, F32) if isinstance(s, tuple) else s for s in scratch],
        compiler_params=pltpu.CompilerParams(vmem_limit_bytes=mib << 20),
    )(*arguments)


def norms_kernel(count, parts, out):
    root = jnp.sqrt(jnp.sum(parts[...], axis=0, keepdims=True) * (1.0 / count))
    out[0] = root[0, 0]
    out[1] = root[0, 1]


def on_device(right_side, damage):
    n = lax.axis_size(ALL)
    slab = (4, W, 16, 128)
    f, *x_sends = call(
        x_pack_kernel,
        ((4, 16, 16, 128), slab, slab),
        tuple(pltpu.with_memory_space_constraint(x, pltpu.HBM) for x in (right_side, damage)),
        8,
        (
            pltpu.VMEM((16, 16, 128), jnp.int32),
            pltpu.SemaphoreType.DMA(()),
            pltpu.SemaphoreType.DMA(()),
        ),
        source=HBM,
    )
    x_pieces = swaps(*x_sends, GX)
    slab = (4, NP // 2, 8, 128)
    y_sends = call(y_pack_kernel, (slab, slab), (f, *x_pieces), 8)
    y_pieces = swaps(*y_sends, "gy")
    pieces = (f, *x_pieces, *y_pieces)
    side = (4, NP, 128)
    z_sends = call(z_pack_kernel, (side, side), pieces, 8)
    z_pieces = swaps(*z_sends, GZ)
    field = (NP, 4, ROWS, 128)
    tails = (4, 4, ROWS, 128)
    edges = (6, ROWS, 128)
    (pq,) = call(main_kernel, (field,), pieces, 8)
    x2, tail, tail_pq, sums = call(
        first_kernel,
        (field, tails, tails, (n, 128)),
        (pq, f, *z_sends, *z_pieces),
        12,
        (edges,),
    )
    every = lax.all_to_all(sums, ALL, 0, 0, tiled=True)
    displacement, partial_sums = call(
        second_kernel,
        (right_side.shape, (n, 128)),
        (every, x2, tail, pq, tail_pq, f),
        20,
        (field, field, tails, tails, (3, 3, ROWS, 128), edges, pltpu.SemaphoreType.DMA((3,))),
        target=(HBM, VMEM),
    )
    partial_sums = lax.all_to_all(partial_sums, ALL, 0, 0, tiled=True)
    (norms,) = call(
        functools.partial(norms_kernel, right_side.size * n), ((2,),), (partial_sums,), 2, target=SMEM
    )
    return (displacement, norms)


def solution(mesh):
    torus = Mesh(mesh.devices.reshape(4, 2, mesh.shape["gy"], 2, 4), ALL)
    placed = (P(None, GX, "gy", GZ), P(GX, "gy", GZ))
    return jax.shard_map(
        on_device,
        mesh=torus,
        in_specs=placed,
        out_specs=(P(None, GX, "gy", GZ), P()),
        check_vma=False,
    )
```

```python
import functools

import jax
import jax.numpy as jnp
from jax import lax
from jax.experimental import pallas as pl
from jax.experimental.pallas import tpu as pltpu
from jax.sharding import Mesh
from jax.sharding import PartitionSpec as P

BLOCK = 16
COARSE = 8
GX = ("gx_0", "gx_1")
GZ = ("gz_0", "gz_1")
ALL = ("gx_0", "gx_1", "gy", "gz_0", "gz_1")

FLOOR_STIFFNESS = 0.05
MASS_TERM = 0.001
COUPLING = 2.5
RELAXATION = 0.6

W = 4
NP = 16 + 2 * W
ROWS = 40
GROUPS = (4, 12, 20)
OWN_GROUPS = (8, 16)
DIAG = 6.0 + 2.0 * COUPLING
OWN = 1.0 + COUPLING
MIX = 0.25 * COUPLING
KEEP = 1.0 - RELAXATION
F32 = jnp.float32


def lanes_of(shape):
    return lax.broadcasted_iota(jnp.int32, shape, 1)


def rows_of(shape):
    return lax.broadcasted_iota(jnp.int32, shape, 0)


def stiffness_of(damage):
    level = damage.astype(F32) / 15.0
    return (1.0 - level) ** 2 * (1.0 - FLOOR_STIFFNESS) + FLOOR_STIFFNESS


def position(axis):
    at = lax.axis_index(axis)
    return at, lax.axis_size(axis), at % 2


def pick(odd, when_odd, when_even):
    return jnp.where(odd, when_odd, when_even)


def tail_parts(tail, row, page):
    v = [tail[page, c, pl.ds(row, 8), :] for c in range(3)]
    yp = [tail[page, c, pl.ds(row + 1, 8), :] for c in range(3)]
    ym = [tail[page, c, pl.ds(row - 1, 8), :] for c in range(3)]
    xp = [pltpu.roll(v[c], 128 - W, 1) for c in range(3)]
    xm = [pltpu.roll(v[c], W, 1) for c in range(3)]
    zx = MIX * (xp[2] - xm[2])
    zy = MIX * (yp[2] - ym[2])
    zz = MIX * ((xp[0] - xm[0]) + (yp[1] - ym[1]))
    own = OWN * v[2]
    ups = (v[0] + zx, v[1] + zy, own + zz)
    downs = (v[0] - zx, v[1] - zy, own - zz)
    return ups, downs, v, xp, xm, yp, ym


def tail_sums(source, row, low):
    lane = lanes_of((8, 128))
    parts = [tail_parts(source, row, page) for page in (low, low + 1)]
    (up_a, down_a), (up_b, down_b) = (part[:2] for part in parts)
    first = lane % W == 0
    last = lane % W == W - 1
    beside_z = (
        [
            jnp.where(last, pltpu.roll(up_b[c], W - 1, 1), pltpu.roll(up_a[c], 127, 1))
            + pltpu.roll(down_a[c], 1, 1)
            for c in range(3)
        ],
        [
            jnp.where(first, pltpu.roll(down_a[c], 129 - W, 1), pltpu.roll(down_b[c], 1, 1))
            + pltpu.roll(up_b[c], 127, 1)
            for c in range(3)
        ],
    )
    sums = []
    for t in range(2):
        _, _, v, xp, xm, yp, ym = parts[t]
        dy0 = MIX * (yp[0] - ym[0])
        dy1 = MIX * (yp[1] - ym[1])
        mix_x = pltpu.roll(dy1, 128 - W, 1) - pltpu.roll(dy1, W, 1)
        mix_y = pltpu.roll(dy0, 128 - W, 1) - pltpu.roll(dy0, W, 1)
        rest = (
            OWN * (xp[0] + xm[0]) + (yp[0] + ym[0]) + mix_x,
            OWN * (yp[1] + ym[1]) + (xp[1] + xm[1]) + mix_y,
            (xp[2] + xm[2]) + (yp[2] + ym[2]),
        )
        sums.append([rest[c] + beside_z[t][c] for c in range(3)])
    return sums, [part[2] for part in parts], up_b, down_a


def put_edges(edges, row, ups, downs):
    last = lanes_of((8, 128)) % W == W - 1
    for c in range(3):
        edges[c, pl.ds(row, 8), :] = jnp.where(
            last, pltpu.roll(ups[c], 127, 1), pltpu.roll(downs[c], 129 - W, 1)
        )


def tail_sweep(source, target, pq, edges=None, outer_only=False):
    for row in GROUPS:
        kept = {}
        for low in (0, 2):
            sums, v, up_b, down_a = tail_sums(source, row, low)
            kept[low] = up_b, down_a
            for t in range(2):
                if outer_only and low + t in (1, 2):
                    continue
                q = pq[low + t, 3, pl.ds(row, 8), :]
                for c in range(3):
                    p = pq[low + t, c, pl.ds(row, 8), :]
                    target[low + t, c, pl.ds(row, 8), :] = KEEP * v[t][c] + p + q * sums[t][c]
        if edges is not None:
            put_edges(edges, row, kept[2][0], kept[0][1])


def edges_only(source, edges):
    for row in OWN_GROUPS:
        put_edges(
            edges, row, tail_parts(source, row, 3)[0], tail_parts(source, row, 0)[1]
        )


def neighbour_sum(ref, edges, i, row, lane):
    def at(c, dx, dy):
        return ref[i + dx, c, pl.ds(row + dy, 8), :]

    v = [at(c, 0, 0) for c in range(3)]
    xp = [at(c, 1, 0) for c in range(3)]
    xm = [at(c, -1, 0) for c in range(3)]
    yp = [at(c, 0, 1) for c in range(3)]
    ym = [at(c, 0, -1) for c in range(3)]
    zx = MIX * (xp[2] - xm[2])
    zy = MIX * (yp[2] - ym[2])
    zz = MIX * ((xp[0] - xm[0]) + (yp[1] - ym[1]))
    own = OWN * v[2]
    ups = (v[0] + zx, v[1] + zy, own + zz)
    downs = (v[0] - zx, v[1] - zy, own - zz)
    mix_x = (at(1, 1, 1) - at(1, 1, -1)) - (at(1, -1, 1) - at(1, -1, -1))
    mix_y = (at(0, 1, 1) - at(0, 1, -1)) - (at(0, -1, 1) - at(0, -1, -1))
    rest = (
        OWN * (xp[0] + xm[0]) + (yp[0] + ym[0]) + MIX * mix_x,
        OWN * (yp[1] + ym[1]) + (xp[1] + xm[1]) + MIX * mix_y,
        (xp[2] + xm[2]) + (yp[2] + ym[2]),
    )
    sums = []
    for c in range(3):
        up, down = pltpu.roll(ups[c], 127, 1), pltpu.roll(downs[c], 1, 1)
        if edges is not None:
            edge = pltpu.roll(edges[c, pl.ds(row, 8), :], 128 - W * i, 1)
            up = jnp.where(lane == 127, edge, up)
            down = jnp.where(lane == 0, edge, down)
        sums.append(rest[c] + (up + down))
    return sums, v


def planes(first, last, body, carry=0):
    whole = first + (last - first) // 4 * 4

    def four(k, carry):
        for j in range(4):
            carry = body(first + 4 * k + j, carry)
        return carry

    carry = lax.fori_loop(0, (last - first) // 4, four, carry)
    for i in range(whole, last):
        carry = body(i, carry)
    return carry


def sweep(source, target, pq, edges, first, last):
    lane = lanes_of((8, 128))

    def plane(i, carry):
        for row in GROUPS:
            sums, v = neighbour_sum(source, edges, i, row, lane)
            q = pq[i, 3, pl.ds(row, 8), :]
            for c in range(3):
                p = pq[i, c, pl.ds(row, 8), :]
                target[i, c, pl.ds(row, 8), :] = KEEP * v[c] + p + q * sums[c]
        return carry

    planes(first, last, plane)


def x_pack_kernel(load, damage, f_out, far_out, near_out, level, load_sem, level_sem):
    odd = position(GX)[2] == 1
    load_copy = pltpu.make_async_copy(load, f_out.at[pl.ds(0, 3)], load_sem)
    level_copy = pltpu.make_async_copy(damage, level, level_sem)
    load_copy.start()
    level_copy.start()
    level_copy.wait()
    f_out[3] = level[...].astype(F32)
    load_copy.wait()
    for c in range(4):
        for i in range(W):
            low, high = f_out[c, i], f_out[c, i + 16 - W]
            far_out[c, i] = pick(odd, high, low)
            near_out[c, i] = pick(odd, low, high)


def y_pack_kernel(f, xfar, xnear, far_out, near_out):
    odd_x, odd_y = position(GX)[2] == 1, position("gy")[2] == 1
    upper = rows_of((8, 128)) < 4

    def tile(c, i, k):
        rows = pl.ds(8 * k, 8)
        if i < W:
            return pick(odd_x, xnear[c, i, rows, :], xfar[c, i, rows, :])
        if i >= W + 16:
            return pick(odd_x, xfar[c, i - W - 16, rows, :], xnear[c, i - W - 16, rows, :])
        return f[c, i - W, rows, :]

    for c in range(4):
        for j in range(NP // 2):
            a, b = 2 * j, 2 * j + 1
            low = jnp.where(upper, tile(c, a, 0), pltpu.roll(tile(c, b, 0), 4, 0))
            high = jnp.where(upper, pltpu.roll(tile(c, a, 1), 4, 0), tile(c, b, 1))
            far_out[c, j] = pick(odd_y, high, low)
            near_out[c, j] = pick(odd_y, low, high)


def z_pack_kernel(f, xfar, xnear, yfar, ynear, far_out, near_out):
    odd_x, odd_y, odd_z = position(GX)[2] == 1, position("gy")[2] == 1, position(GZ)[2]
    lane = lanes_of((8, 128))
    upper = rows_of((8, 128)) < 4
    for c in range(4):
        for k in range(3):
            far = jnp.zeros((8, 128), F32)
            near = far
            for i in range(NP):
                if k == 2:
                    low = pick(odd_y, ynear[c, i // 2], yfar[c, i // 2])
                    high = pick(odd_y, yfar[c, i // 2], ynear[c, i // 2])
                    if i % 2:
                        value = jnp.where(upper, pltpu.roll(low, 4, 0), high)
                    else:
                        value = jnp.where(upper, low, pltpu.roll(high, 4, 0))
                else:
                    rows = pl.ds(8 * k, 8)
                    if i < W:
                        value = pick(odd_x, xnear[c, i, rows, :], xfar[c, i, rows, :])
                    elif i >= W + 16:
                        j = i - W - 16
                        value = pick(odd_x, xfar[c, j, rows, :], xnear[c, j, rows, :])
                    else:
                        value = f[c, i - W, rows, :]
                here = (lane >= W * i) & (lane < W * i + W)
                far = jnp.where(here, pltpu.roll(value, W * i + W * odd_z, 1), far)
                near = jnp.where(here, pltpu.roll(value, W * i + W * (1 - odd_z), 1), near)
            far_out[c, pl.ds(8 * k, 8), :] = far
            near_out[c, pl.ds(8 * k, 8), :] = near


def main_kernel(f, xfar, xnear, yfar, ynear, pq, x2, columns):
    gx, gx_n, odd_x = position(GX)
    gy, gy_n, odd_y = position("gy")
    odd_x, odd_y = odd_x == 1, odd_y == 1

    def x_inside(i):
        x = gx * 16 + i - W
        return (x >= 0) & (x < gx_n * 16)

    def values(parts, inside):
        g = stiffness_of(parts[3])
        scale = RELAXATION / (g * DIAG + MASS_TERM)
        out = [part * scale for part in parts[:3]] + [g * scale]
        return [jnp.where(inside, value, 0.0) for value in out]

    def fill(i, parts):
        for c, value in enumerate(values(parts, x_inside(i))):
            pq[i, c, pl.ds(8, 16), :] = value

    def own(i, carry):
        fill(i, [f[c, i - W] for c in range(4)])
        return carry

    lax.fori_loop(W, W + 16, own, 0)

    def beside_x(i, carry):
        fill(i, [pick(odd_x, xnear[c, i], xfar[c, i]) for c in range(4)])
        fill(i + W + 16, [pick(odd_x, xfar[c, i], xnear[c, i]) for c in range(4)])
        return carry

    lax.fori_loop(0, W, beside_x, 0)
    second = (rows_of((8, 128)) >= 4).astype(jnp.int32)
    low_in, high_in = gy > 0, gy < gy_n - 1

    def beside_y(j, carry):
        inside = x_inside(2 * j + second)
        low = values([pick(odd_y, ynear[c, j], yfar[c, j]) for c in range(4)], inside & low_in)
        high = values([pick(odd_y, yfar[c, j], ynear[c, j]) for c in range(4)], inside & high_in)
        for c in range(4):
            for t in range(2):
                pq[2 * j + t, c, pl.ds(4, 4), :] = low[c][4 * t : 4 * t + 4]
                pq[2 * j + t, c, pl.ds(24, 4), :] = high[c][4 * t : 4 * t + 4]
        return carry

    lax.fori_loop(0, NP // 2, beside_y, 0)
    sweep(pq, x2, pq, None, 1, NP - 1)
    lane = lanes_of((8, 128))
    row8 = rows_of((8, 128))

    def residual(i, carry):
        totals = list(carry)
        for row in OWN_GROUPS:
            sums, v = neighbour_sum(x2, None, i, row, lane)
            rows = pl.ds(row - 8, 8)
            g = stiffness_of(f[3, i - W, rows, :])
            d = g * DIAG + MASS_TERM
            for c in range(3):
                load = f[c, i - W, rows, :]
                totals[c] += (load - d * v[c]) + g * sums[c]
                totals[4] += load * load
            totals[3] += g
        return tuple(totals)

    zero = jnp.zeros((8, 128), F32)
    totals = planes(W, W + 16, residual, (zero,) * 5)
    stacked = zero
    inner = (lane >= 2) & (lane < 126)
    for c in range(5):
        total = jnp.where(inner, totals[c], 0.0) if c < 3 else totals[c]
        stacked = jnp.where(row8 == c, jnp.sum(total, axis=0, keepdims=True), stacked)
    columns[...] = stacked


def first_kernel(columns, zfar_own, znear_own, zfar, znear, tail, tail_pq, sums_out):
    lane = lanes_of((8, 128))
    row8 = rows_of((8, 128))
    gx, gx_n, _ = position(GX)
    gy, gy_n, _ = position("gy")
    gz, gz_n, odd_z = position(GZ)
    odd_z = odd_z == 1
    x = gx * 16 + lane // W - W
    x_in = (x >= 0) & (x < gx_n * 16)
    y_in = ((row8 >= 4) | (gy > 0)) & ((row8 < 4) | (gy < gy_n - 1))
    z_in = (gz > 0, True, True, gz < gz_n - 1)
    sides = (
        (znear, zfar),
        (znear_own, zfar_own),
        (zfar_own, znear_own),
        (zfar, znear),
    )

    def part(page, c, k):
        when_odd, when_even = sides[page]
        rows = pl.ds(8 * k, 8)
        return pick(odd_z, when_odd[c, rows, :], when_even[c, rows, :])

    for page in range(4):
        for k in range(3):
            g = stiffness_of(part(page, 3, k))
            scale = RELAXATION / (g * DIAG + MASS_TERM)
            inside = x_in
            if page in (0, 3):
                inside = inside & z_in[page]
            if k == 2:
                inside = inside & y_in
            for c in range(4):
                value = jnp.where(inside, (part(page, c, k) if c < 3 else g) * scale, 0.0)
                if k < 2:
                    tail_pq[page, c, pl.ds(8 + 8 * k, 8), :] = value
                else:
                    tail_pq[page, c, pl.ds(4, 4), :] = value[:4]
                    tail_pq[page, c, pl.ds(24, 4), :] = value[4:]
    tail_sweep(tail_pq, tail, tail_pq)
    zero = jnp.zeros((8, 128), F32)
    ends = zero
    for side in range(2):
        page = 1 + side
        here = (lane % W < 2) if side == 0 else (lane % W >= 2)
        totals = [zero] * 3
        for row in OWN_GROUPS:
            sums, v, _, _ = tail_sums(tail, row, 2 * side)
            k = row // 8 - 1
            g = stiffness_of(part(page, 3, k))
            d = g * DIAG + MASS_TERM
            for c in range(3):
                totals[c] += (part(page, c, k) - d * v[1 - side][c]) + g * sums[1 - side][c]
        for c in range(3):
            total = jnp.sum(jnp.where(here, totals[c], 0.0), axis=0, keepdims=True)
            ends = jnp.where(row8 == 3 * side + c, total, ends)
    big = (128, 128)
    gather = (rows_of(big) // BLOCK == lanes_of(big) % 8).astype(F32)
    own = ((rows_of(big) >= W * W) & (rows_of(big) < W * (W + 16))).astype(F32)

    def dot(a, b):
        return jnp.dot(a, b, precision=lax.Precision.HIGHEST, preferred_element_type=F32)

    ends = jnp.where((lane >= W * W) & (lane < W * (W + 16)), ends, 0.0)
    by_cell = dot(columns[...], gather)
    by_end = dot(ends, own)
    low_end = (lane % 8 == 0) & (lane // 8 == row8) & (row8 < 3)
    high_end = (lane % 8 == 7) & (lane // 8 + 3 == row8) & (row8 < 6)
    slot = jnp.where(lane // 8 == row8, by_cell, 0.0) + jnp.where(
        low_end | high_end, by_end, 0.0
    )
    sums_out[...] = jnp.broadcast_to(jnp.sum(slot, axis=0, keepdims=True), sums_out.shape)


def coarse_solve(load, mean, gx_n, gy_n, gz_n):
    shape = load[0].shape
    n = shape[1]
    lane = lanes_of(shape)
    row = rows_of(shape)
    sx, sy = gy_n * gz_n, gz_n
    x_at, y_at, z_at = lane // sx, lane // sy % gy_n, lane % gz_n

    def shift(v, step, at, count):
        up = jnp.where(at < count - 1, pltpu.roll(v, n - step, 1), 0.0)
        down = jnp.where(at > 0, pltpu.roll(v, step, 1), 0.0)
        return up, down

    def shift_z(v):
        up = pltpu.roll(v, 7, 0)
        down = pltpu.roll(v, 1, 0)
        next_up = jnp.where(z_at < gz_n - 1, pltpu.roll(up, n - 1, 1), 0.0)
        next_down = jnp.where(z_at > 0, pltpu.roll(down, 1, 1), 0.0)
        return jnp.where(row == 7, next_up, up), jnp.where(row == 0, next_down, down)

    shifts = (
        lambda v: shift(v, sx, x_at, gx_n),
        lambda v: shift(v, sy, y_at, gy_n),
        shift_z,
    )
    coefficient = BLOCK**2 * mean
    scale = RELAXATION / (coefficient * DIAG + BLOCK**3 * MASS_TERM)
    p = [scale * value for value in load]
    q = scale * coefficient

    def step(_, w):
        pairs = [[shifts[b](w[a]) for b in range(3)] for a in range(3)]
        diffs = [pairs[a][a][0] - pairs[a][a][1] for a in range(3)]
        out = []
        for a in range(3):
            total = 0.0
            for b in range(3):
                both = pairs[a][b][0] + pairs[a][b][1]
                total = total + (OWN * both if a == b else both)
            others = [diffs[b] for b in range(3) if b != a]
            up, down = shifts[a](others[0] + others[1])
            out.append(KEEP * w[a] + p[a] + q * (total + MIX * (up - down)))
        return tuple(out)

    return lax.fori_loop(0, COARSE - 1, step, tuple(p))


def second_kernel(
    every,
    x2,
    tail2,
    pq,
    tail_pq,
    f,
    out,
    sum_out,
    x3,
    x4,
    tail3,
    tail4,
    w_ref,
    edges,
    out_sem,
):
    gx, gx_n, _ = position(GX)
    gy, gy_n, _ = position("gy")
    gz, gz_n, _ = position(GZ)
    me = (gx * gy_n + gy) * gz_n + gz
    lane = lanes_of((8, 128))
    row8 = rows_of((8, 128))
    cells = jnp.transpose(every[...])
    load = [cells[8 * c : 8 * c + 8] for c in range(3)]
    mean = cells[24:32] * (1.0 / BLOCK**3)
    load_sum = jnp.sum(cells[32:40])
    w = coarse_solve(load, mean, gx_n, gy_n, gz_n)
    n = gx_n * gy_n * gz_n
    centre = n // 2
    own_cells = (lane // BLOCK == row8).astype(F32)
    line = lane[:1]
    cell_of = ((7, -1), (0, 0), (7, 0), (0, 1))
    spans = ((4, 4), (8, 16), (24, 4))
    for c in range(3):
        turned = pltpu.roll(w[c], (centre + n - me) % n, 1)

        def column(dx, dy):
            return centre + (dx - 1) * gy_n * gz_n + (dy - 1) * gz_n

        for dy in range(3):
            first, size = spans[dy]
            for dx in range(3):
                j = column(dx, dy)
                main = jnp.sum(turned[:, j : j + 1] * own_cells, axis=0, keepdims=True)
                w_ref[dx, c, pl.ds(first, size), :] = jnp.broadcast_to(main, (size, 128))
            for page in range(4):
                k, dz = cell_of[page]
                here = [
                    jnp.broadcast_to(
                        turned[k : k + 1, column(dx, dy) + dz : column(dx, dy) + dz + 1], (1, 128)
                    )
                    for dx in range(3)
                ]
                value = jnp.where(
                    line < W * W, here[0], jnp.where(line < W * (W + 16), here[1], here[2])
                )
                rows = pl.ds(first, size)
                inside = tail_pq[page, 3, rows, :] > 0.0
                tail3[page, c, rows, :] = tail2[page, c, rows, :] + jnp.where(inside, value, 0.0)

    ends = (lane == 0) | (lane == 127)
    for row in GROUPS:
        for c in range(3):
            rows = pl.ds(row, 8)
            edges[c, rows, :] = jnp.where(
                lane % W == W - 1, pltpu.roll(tail3[2, c, rows, :], 128 - W, 1), tail3[1, c, rows, :]
            )

    def correct(i, carry):
        cell = (i >= W) * 1 + (i >= W + 16) * 1
        for row in GROUPS:
            rows = pl.ds(row, 8)
            inside = pq[i, 3, rows, :] > 0.0
            for c in range(3):
                edge = pltpu.roll(edges[c, rows, :], 128 - W * i, 1)
                value = x2[i, c, rows, :] + jnp.where(inside, w_ref[cell, c, rows, :], 0.0)
                x3[i, c, rows, :] = jnp.where(ends, edge, value)
        return carry

    planes(1, NP - 1, correct)
    tail_sweep(tail3, tail4, tail_pq, edges)
    sweep(x3, x4, pq, edges, 2, NP - 2)
    tail_sweep(tail4, tail3, tail_pq, edges, True)
    sweep(x4, x3, pq, edges, 3, NP - 3)
    copies = [
        pltpu.make_async_copy(
            x3.at[pl.ds(W, 16), c, pl.ds(8, 16), :], out.at[c], out_sem.at[c]
        )
        for c in range(3)
    ]
    for copy in copies:
        copy.start()
    edges_only(tail3, edges)

    def residual(i, total):
        for row in OWN_GROUPS:
            sums, v = neighbour_sum(x3, edges, i, row, lane)
            rows = pl.ds(row - 8, 8)
            g = stiffness_of(f[3, i - W, rows, :])
            d = (g * DIAG + MASS_TERM) * (1.0 / RELAXATION)
            q = pq[i, 3, pl.ds(row, 8), :]
            for c in range(3):
                p = pq[i, c, pl.ds(row, 8), :]
                r = d * ((p - RELAXATION * v[c]) + q * sums[c])
                total += r * r
        return total

    total = jnp.sum(planes(W, W + 16, residual, jnp.zeros((8, 128), F32)))
    both = jnp.where(line == 0, load_sum * (1.0 / n), total)
    sum_out[...] = jnp.broadcast_to(both, sum_out.shape)
    for copy in copies:
        copy.wait()


def swaps(far_send, near_send, axis):
    count = lax.axis_size(axis)
    near = [(i, i ^ 1) for i in range(count)]
    far = [(i, ((i ^ 1) + (2 if i % 2 else -2)) % count) for i in range(count)]
    return lax.ppermute(far_send, axis, far), lax.ppermute(near_send, axis, near)


VMEM = pl.BlockSpec(memory_space=pltpu.VMEM)
SMEM = pl.BlockSpec(memory_space=pltpu.SMEM)
HBM = pl.BlockSpec(memory_space=pltpu.HBM)


def call(kernel, shapes, arguments, mib, scratch=(), source=VMEM, target=VMEM):
    shapes = [jax.ShapeDtypeStruct(shape, F32) for shape in shapes]
    return pl.pallas_call(
        kernel,
        out_shape=tuple(shapes),
        in_specs=[source] * len(arguments),
        out_specs=target if isinstance(target, tuple) else (target,) * len(shapes),
        scratch_shapes=[pltpu.VMEM(s, F32) if isinstance(s, tuple) else s for s in scratch],
        compiler_params=pltpu.CompilerParams(vmem_limit_bytes=mib << 20),
    )(*arguments)


def norms_kernel(count, parts, out):
    root = jnp.sqrt(jnp.sum(parts[...], axis=0, keepdims=True) * (1.0 / count))
    out[0] = root[0, 0]
    out[1] = root[0, 1]


def on_device(right_side, damage):
    n = lax.axis_size(ALL)
    slab = (4, W, 16, 128)
    f, *x_sends = call(
        x_pack_kernel,
        ((4, 16, 16, 128), slab, slab),
        tuple(pltpu.with_memory_space_constraint(x, pltpu.HBM) for x in (right_side, damage)),
        8,
        (
            pltpu.VMEM((16, 16, 128), jnp.int32),
            pltpu.SemaphoreType.DMA(()),
            pltpu.SemaphoreType.DMA(()),
        ),
        source=HBM,
    )
    x_pieces = swaps(*x_sends, GX)
    slab = (4, NP // 2, 8, 128)
    y_sends = call(y_pack_kernel, (slab, slab), (f, *x_pieces), 8)
    y_pieces = swaps(*y_sends, "gy")
    pieces = (f, *x_pieces, *y_pieces)
    side = (4, NP, 128)
    z_sends = call(z_pack_kernel, (side, side), pieces, 8)
    z_pieces = swaps(*z_sends, GZ)
    field = (NP, 4, ROWS, 128)
    tails = (4, 4, ROWS, 128)
    edges = (3, ROWS, 128)
    pq, x2, columns = call(main_kernel, (field, field, (8, 128)), pieces, 12)
    tail, tail_pq, sums = call(
        first_kernel, (tails, tails, (n, 128)), (columns, *z_sends, *z_pieces), 8
    )
    every = lax.all_to_all(sums, ALL, 0, 0, tiled=True)
    displacement, partial_sums = call(
        second_kernel,
        (right_side.shape, (n, 128)),
        (every, x2, tail, pq, tail_pq, f),
        20,
        (field, field, tails, tails, (3, 3, ROWS, 128), edges, pltpu.SemaphoreType.DMA((3,))),
        target=(HBM, VMEM),
    )
    partial_sums = lax.all_to_all(partial_sums, ALL, 0, 0, tiled=True)
    (norms,) = call(
        functools.partial(norms_kernel, right_side.size * n), ((2,),), (partial_sums,), 2, target=SMEM
    )
    return (displacement, norms)


def solution(mesh):
    torus = Mesh(mesh.devices.reshape(4, 2, mesh.shape["gy"], 2, 4), ALL)
    placed = (P(None, GX, "gy", GZ), P(GX, "gy", GZ))
    return jax.shard_map(
        on_device,
        mesh=torus,
        in_specs=placed,
        out_specs=(P(None, GX, "gy", GZ), P()),
        check_vma=False,
    )
```

```python
import functools

import jax
import jax.numpy as jnp
from jax import lax
from jax.experimental import pallas as pl
from jax.experimental.pallas import tpu as pltpu
from jax.sharding import Mesh
from jax.sharding import PartitionSpec as P

BLOCK = 16
COARSE = 8
GX = ("gx_0", "gx_1")
GZ = ("gz_0", "gz_1")
ALL = ("gx_0", "gx_1", "gy", "gz_0", "gz_1")

FLOOR_STIFFNESS = 0.05
MASS_TERM = 0.001
COUPLING = 2.5
RELAXATION = 0.6

W = 4
NP = 16 + 2 * W
ROWS = 40
GROUPS = (4, 12, 20)
OWN_GROUPS = (8, 16)
DIAG = 6.0 + 2.0 * COUPLING
OWN = 1.0 + COUPLING
MIX = 0.25 * COUPLING
KEEP = 1.0 - RELAXATION
F32 = jnp.float32


def lanes_of(shape):
    return lax.broadcasted_iota(jnp.int32, shape, 1)


def rows_of(shape):
    return lax.broadcasted_iota(jnp.int32, shape, 0)


def stiffness_of(damage):
    level = damage.astype(F32) / 15.0
    return (1.0 - level) ** 2 * (1.0 - FLOOR_STIFFNESS) + FLOOR_STIFFNESS


def position(axis):
    at = lax.axis_index(axis)
    return at, lax.axis_size(axis), at % 2


def pick(odd, when_odd, when_even):
    return jnp.where(odd, when_odd, when_even)


def tail_parts(tail, row, page):
    v = [tail[page, c, pl.ds(row, 8), :] for c in range(3)]
    yp = [tail[page, c, pl.ds(row + 1, 8), :] for c in range(3)]
    ym = [tail[page, c, pl.ds(row - 1, 8), :] for c in range(3)]
    xp = [pltpu.roll(v[c], 128 - W, 1) for c in range(3)]
    xm = [pltpu.roll(v[c], W, 1) for c in range(3)]
    zx = MIX * (xp[2] - xm[2])
    zy = MIX * (yp[2] - ym[2])
    zz = MIX * ((xp[0] - xm[0]) + (yp[1] - ym[1]))
    own = OWN * v[2]
    ups = (v[0] + zx, v[1] + zy, own + zz)
    downs = (v[0] - zx, v[1] - zy, own - zz)
    return ups, downs, v, xp, xm, yp, ym


def tail_sums(source, row, low):
    lane = lanes_of((8, 128))
    parts = [tail_parts(source, row, page) for page in (low, low + 1)]
    (up_a, down_a), (up_b, down_b) = (part[:2] for part in parts)
    first = lane % W == 0
    last = lane % W == W - 1
    beside_z = (
        [
            jnp.where(last, pltpu.roll(up_b[c], W - 1, 1), pltpu.roll(up_a[c], 127, 1))
            + pltpu.roll(down_a[c], 1, 1)
            for c in range(3)
        ],
        [
            jnp.where(first, pltpu.roll(down_a[c], 129 - W, 1), pltpu.roll(down_b[c], 1, 1))
            + pltpu.roll(up_b[c], 127, 1)
            for c in range(3)
        ],
    )
    sums = []
    for t in range(2):
        _, _, v, xp, xm, yp, ym = parts[t]
        dy0 = MIX * (yp[0] - ym[0])
        dy1 = MIX * (yp[1] - ym[1])
        mix_x = pltpu.roll(dy1, 128 - W, 1) - pltpu.roll(dy1, W, 1)
        mix_y = pltpu.roll(dy0, 128 - W, 1) - pltpu.roll(dy0, W, 1)
        rest = (
            OWN * (xp[0] + xm[0]) + (yp[0] + ym[0]) + mix_x,
            OWN * (yp[1] + ym[1]) + (xp[1] + xm[1]) + mix_y,
            (xp[2] + xm[2]) + (yp[2] + ym[2]),
        )
        sums.append([rest[c] + beside_z[t][c] for c in range(3)])
    return sums, [part[2] for part in parts], up_b, down_a


def put_edges(edges, row, ups, downs):
    last = lanes_of((8, 128)) % W == W - 1
    for c in range(3):
        edges[c, pl.ds(row, 8), :] = jnp.where(
            last, pltpu.roll(ups[c], 127, 1), pltpu.roll(downs[c], 129 - W, 1)
        )


def tail_sweep(source, target, pq, edges=None, outer_only=False):
    for row in GROUPS:
        kept = {}
        for low in (0, 2):
            sums, v, up_b, down_a = tail_sums(source, row, low)
            kept[low] = up_b, down_a
            for t in range(2):
                if outer_only and low + t in (1, 2):
                    continue
                q = pq[low + t, 3, pl.ds(row, 8), :]
                for c in range(3):
                    p = pq[low + t, c, pl.ds(row, 8), :]
                    target[low + t, c, pl.ds(row, 8), :] = KEEP * v[t][c] + p + q * sums[t][c]
        if edges is not None:
            put_edges(edges, row, kept[2][0], kept[0][1])


def edges_only(source, edges):
    for row in OWN_GROUPS:
        put_edges(
            edges, row, tail_parts(source, row, 3)[0], tail_parts(source, row, 0)[1]
        )


def neighbour_sum(ref, edges, i, row, lane):
    def at(c, dx, dy):
        return ref[i + dx, c, pl.ds(row + dy, 8), :]

    v = [at(c, 0, 0) for c in range(3)]
    xp = [at(c, 1, 0) for c in range(3)]
    xm = [at(c, -1, 0) for c in range(3)]
    yp = [at(c, 0, 1) for c in range(3)]
    ym = [at(c, 0, -1) for c in range(3)]
    zx = MIX * (xp[2] - xm[2])
    zy = MIX * (yp[2] - ym[2])
    zz = MIX * ((xp[0] - xm[0]) + (yp[1] - ym[1]))
    own = OWN * v[2]
    ups = (v[0] + zx, v[1] + zy, own + zz)
    downs = (v[0] - zx, v[1] - zy, own - zz)
    mix_x = (at(1, 1, 1) - at(1, 1, -1)) - (at(1, -1, 1) - at(1, -1, -1))
    mix_y = (at(0, 1, 1) - at(0, 1, -1)) - (at(0, -1, 1) - at(0, -1, -1))
    rest = (
        OWN * (xp[0] + xm[0]) + (yp[0] + ym[0]) + MIX * mix_x,
        OWN * (yp[1] + ym[1]) + (xp[1] + xm[1]) + MIX * mix_y,
        (xp[2] + xm[2]) + (yp[2] + ym[2]),
    )
    sums = []
    for c in range(3):
        up, down = pltpu.roll(ups[c], 127, 1), pltpu.roll(downs[c], 1, 1)
        if edges is not None:
            edge = pltpu.roll(edges[c, pl.ds(row, 8), :], 128 - W * i, 1)
            up = jnp.where(lane == 127, edge, up)
            down = jnp.where(lane == 0, edge, down)
        sums.append(rest[c] + (up + down))
    return sums, v


def planes(first, last, body, carry=0):
    whole = first + (last - first) // 4 * 4

    def four(k, carry):
        for j in range(4):
            carry = body(first + 4 * k + j, carry)
        return carry

    carry = lax.fori_loop(0, (last - first) // 4, four, carry)
    for i in range(whole, last):
        carry = body(i, carry)
    return carry


def sweep(source, target, pq, edges, first, last):
    lane = lanes_of((8, 128))

    def plane(i, carry):
        for row in GROUPS:
            sums, v = neighbour_sum(source, edges, i, row, lane)
            q = pq[i, 3, pl.ds(row, 8), :]
            for c in range(3):
                p = pq[i, c, pl.ds(row, 8), :]
                target[i, c, pl.ds(row, 8), :] = KEEP * v[c] + p + q * sums[c]
        return carry

    planes(first, last, plane)


def x_pack_kernel(load, damage, f_out, far_out, near_out, level, load_sem, level_sem):
    odd = position(GX)[2] == 1
    load_copy = pltpu.make_async_copy(load, f_out.at[pl.ds(0, 3)], load_sem)
    level_copy = pltpu.make_async_copy(damage, level, level_sem)
    load_copy.start()
    level_copy.start()
    level_copy.wait()
    f_out[3] = level[...].astype(F32)
    load_copy.wait()
    for c in range(4):
        for i in range(W):
            low, high = f_out[c, i], f_out[c, i + 16 - W]
            far_out[c, i] = pick(odd, high, low)
            near_out[c, i] = pick(odd, low, high)


def y_pack_kernel(f, xfar, xnear, far_out, near_out):
    odd_x, odd_y = position(GX)[2] == 1, position("gy")[2] == 1
    upper = rows_of((8, 128)) < 4

    def tile(c, i, k):
        rows = pl.ds(8 * k, 8)
        if i < W:
            return pick(odd_x, xnear[c, i, rows, :], xfar[c, i, rows, :])
        if i >= W + 16:
            return pick(odd_x, xfar[c, i - W - 16, rows, :], xnear[c, i - W - 16, rows, :])
        return f[c, i - W, rows, :]

    for c in range(4):
        for j in range(NP // 2):
            a, b = 2 * j, 2 * j + 1
            low = jnp.where(upper, tile(c, a, 0), pltpu.roll(tile(c, b, 0), 4, 0))
            high = jnp.where(upper, pltpu.roll(tile(c, a, 1), 4, 0), tile(c, b, 1))
            far_out[c, j] = pick(odd_y, high, low)
            near_out[c, j] = pick(odd_y, low, high)


def put_z_pack(values, rows, odd_z, far_out, near_out):
    lane = lanes_of((8, 128))
    for c in range(4):
        far = jnp.zeros((8, 128), F32)
        near = far
        for i in range(NP):
            value = values(c, i)
            here = (lane >= W * i) & (lane < W * i + W)
            far = jnp.where(here, pltpu.roll(value, W * i + W * odd_z, 1), far)
            near = jnp.where(here, pltpu.roll(value, W * i + W * (1 - odd_z), 1), near)
        far_out[c, rows, :] = far
        near_out[c, rows, :] = near


def z_pack_own_kernel(f, xfar, xnear, far_out, near_out):
    odd_x = position(GX)[2] == 1
    for k in range(2):
        rows = pl.ds(8 * k, 8)

        def values(c, i):
            if i < W:
                return pick(odd_x, xnear[c, i, rows, :], xfar[c, i, rows, :])
            if i >= W + 16:
                j = i - W - 16
                return pick(odd_x, xfar[c, j, rows, :], xnear[c, j, rows, :])
            return f[c, i - W, rows, :]

        put_z_pack(values, rows, position(GZ)[2], far_out, near_out)


def z_pack_kernel(yfar, ynear, far_own, near_own, far_out, near_out):
    odd_y = position("gy")[2] == 1
    upper = rows_of((8, 128)) < 4
    for c in range(4):
        far_out[c, pl.ds(0, 16), :] = far_own[c]
        near_out[c, pl.ds(0, 16), :] = near_own[c]

    def values(c, i):
        low = pick(odd_y, ynear[c, i // 2], yfar[c, i // 2])
        high = pick(odd_y, yfar[c, i // 2], ynear[c, i // 2])
        if i % 2:
            return jnp.where(upper, pltpu.roll(low, 4, 0), high)
        return jnp.where(upper, low, pltpu.roll(high, 4, 0))

    put_z_pack(values, pl.ds(16, 8), position(GZ)[2], far_out, near_out)


def main_kernel(f, xfar, xnear, yfar, ynear, pq, y3, columns, x2):
    gx, gx_n, odd_x = position(GX)
    gy, gy_n, odd_y = position("gy")
    odd_x, odd_y = odd_x == 1, odd_y == 1

    def x_inside(i):
        x = gx * 16 + i - W
        return (x >= 0) & (x < gx_n * 16)

    def values(parts, inside):
        g = stiffness_of(parts[3])
        scale = RELAXATION / (g * DIAG + MASS_TERM)
        out = [part * scale for part in parts[:3]] + [g * scale]
        return [jnp.where(inside, value, 0.0) for value in out]

    def fill(i, parts):
        for c, value in enumerate(values(parts, x_inside(i))):
            pq[i, c, pl.ds(8, 16), :] = value

    def own(i, carry):
        fill(i, [f[c, i - W] for c in range(4)])
        return carry

    lax.fori_loop(W, W + 16, own, 0)

    def beside_x(i, carry):
        fill(i, [pick(odd_x, xnear[c, i], xfar[c, i]) for c in range(4)])
        fill(i + W + 16, [pick(odd_x, xfar[c, i], xnear[c, i]) for c in range(4)])
        return carry

    lax.fori_loop(0, W, beside_x, 0)
    second = (rows_of((8, 128)) >= 4).astype(jnp.int32)
    low_in, high_in = gy > 0, gy < gy_n - 1

    def beside_y(j, carry):
        inside = x_inside(2 * j + second)
        low = values([pick(odd_y, ynear[c, j], yfar[c, j]) for c in range(4)], inside & low_in)
        high = values([pick(odd_y, yfar[c, j], ynear[c, j]) for c in range(4)], inside & high_in)
        for c in range(4):
            for t in range(2):
                pq[2 * j + t, c, pl.ds(4, 4), :] = low[c][4 * t : 4 * t + 4]
                pq[2 * j + t, c, pl.ds(24, 4), :] = high[c][4 * t : 4 * t + 4]
        return carry

    lax.fori_loop(0, NP // 2, beside_y, 0)
    sweep(pq, x2, pq, None, 1, NP - 1)
    lane = lanes_of((8, 128))
    row8 = rows_of((8, 128))

    def residual(i, carry):
        totals = list(carry)
        for row in OWN_GROUPS:
            sums, v = neighbour_sum(x2, None, i, row, lane)
            rows = pl.ds(row - 8, 8)
            g = stiffness_of(f[3, i - W, rows, :])
            d = g * DIAG + MASS_TERM
            for c in range(3):
                load = f[c, i - W, rows, :]
                totals[c] += (load - d * v[c]) + g * sums[c]
                totals[4] += load * load
            totals[3] += g
        return tuple(totals)

    zero = jnp.zeros((8, 128), F32)
    totals = planes(W, W + 16, residual, (zero,) * 5)
    stacked = zero
    inner = (lane >= 2) & (lane < 126)
    for c in range(5):
        total = jnp.where(inner, totals[c], 0.0) if c < 3 else totals[c]
        stacked = jnp.where(row8 == c, jnp.sum(total, axis=0, keepdims=True), stacked)
    columns[...] = stacked
    sweep(x2, y3, pq, None, 2, NP - 2)


def first_kernel(columns, zfar_own, znear_own, zfar, znear, tail, tail_pq, sums_out):
    lane = lanes_of((8, 128))
    row8 = rows_of((8, 128))
    gx, gx_n, _ = position(GX)
    gy, gy_n, _ = position("gy")
    gz, gz_n, odd_z = position(GZ)
    odd_z = odd_z == 1
    x = gx * 16 + lane // W - W
    x_in = (x >= 0) & (x < gx_n * 16)
    y_in = ((row8 >= 4) | (gy > 0)) & ((row8 < 4) | (gy < gy_n - 1))
    z_in = (gz > 0, True, True, gz < gz_n - 1)
    sides = (
        (znear, zfar),
        (znear_own, zfar_own),
        (zfar_own, znear_own),
        (zfar, znear),
    )

    def part(page, c, k):
        when_odd, when_even = sides[page]
        rows = pl.ds(8 * k, 8)
        return pick(odd_z, when_odd[c, rows, :], when_even[c, rows, :])

    for page in range(4):
        for k in range(3):
            g = stiffness_of(part(page, 3, k))
            scale = RELAXATION / (g * DIAG + MASS_TERM)
            inside = x_in
            if page in (0, 3):
                inside = inside & z_in[page]
            if k == 2:
                inside = inside & y_in
            for c in range(4):
                value = jnp.where(inside, (part(page, c, k) if c < 3 else g) * scale, 0.0)
                if k < 2:
                    tail_pq[page, c, pl.ds(8 + 8 * k, 8), :] = value
                else:
                    tail_pq[page, c, pl.ds(4, 4), :] = value[:4]
                    tail_pq[page, c, pl.ds(24, 4), :] = value[4:]
    tail_sweep(tail_pq, tail, tail_pq)
    zero = jnp.zeros((8, 128), F32)
    ends = zero
    for side in range(2):
        page = 1 + side
        here = (lane % W < 2) if side == 0 else (lane % W >= 2)
        totals = [zero] * 3
        for row in OWN_GROUPS:
            sums, v, _, _ = tail_sums(tail, row, 2 * side)
            k = row // 8 - 1
            g = stiffness_of(part(page, 3, k))
            d = g * DIAG + MASS_TERM
            for c in range(3):
                totals[c] += (part(page, c, k) - d * v[1 - side][c]) + g * sums[1 - side][c]
        for c in range(3):
            total = jnp.sum(jnp.where(here, totals[c], 0.0), axis=0, keepdims=True)
            ends = jnp.where(row8 == 3 * side + c, total, ends)
    big = (128, 128)
    gather = (rows_of(big) // BLOCK == lanes_of(big) % 8).astype(F32)
    own = ((rows_of(big) >= W * W) & (rows_of(big) < W * (W + 16))).astype(F32)

    def dot(a, b):
        return jnp.dot(a, b, precision=lax.Precision.HIGHEST, preferred_element_type=F32)

    ends = jnp.where((lane >= W * W) & (lane < W * (W + 16)), ends, 0.0)
    by_cell = dot(columns[...], gather)
    by_end = dot(ends, own)
    low_end = (lane % 8 == 0) & (lane // 8 == row8) & (row8 < 3)
    high_end = (lane % 8 == 7) & (lane // 8 + 3 == row8) & (row8 < 6)
    slot = jnp.where(lane // 8 == row8, by_cell, 0.0) + jnp.where(
        low_end | high_end, by_end, 0.0
    )
    sums_out[...] = jnp.broadcast_to(jnp.sum(slot, axis=0, keepdims=True), sums_out.shape)


def coarse_solve(load, mean, gx_n, gy_n, gz_n):
    shape = load[0].shape
    n = shape[1]
    lane = lanes_of(shape)
    row = rows_of(shape)
    sx, sy = gy_n * gz_n, gz_n
    x_at, y_at, z_at = lane // sx, lane // sy % gy_n, lane % gz_n

    def shift(v, step, at, count):
        up = jnp.where(at < count - 1, pltpu.roll(v, n - step, 1), 0.0)
        down = jnp.where(at > 0, pltpu.roll(v, step, 1), 0.0)
        return up, down

    def shift_z(v):
        up = pltpu.roll(v, 7, 0)
        down = pltpu.roll(v, 1, 0)
        next_up = jnp.where(z_at < gz_n - 1, pltpu.roll(up, n - 1, 1), 0.0)
        next_down = jnp.where(z_at > 0, pltpu.roll(down, 1, 1), 0.0)
        return jnp.where(row == 7, next_up, up), jnp.where(row == 0, next_down, down)

    shifts = (
        lambda v: shift(v, sx, x_at, gx_n),
        lambda v: shift(v, sy, y_at, gy_n),
        shift_z,
    )
    coefficient = BLOCK**2 * mean
    scale = RELAXATION / (coefficient * DIAG + BLOCK**3 * MASS_TERM)
    p = [scale * value for value in load]
    q = scale * coefficient

    def step(_, w):
        pairs = [[shifts[b](w[a]) for b in range(3)] for a in range(3)]
        diffs = [pairs[a][a][0] - pairs[a][a][1] for a in range(3)]
        out = []
        for a in range(3):
            total = 0.0
            for b in range(3):
                both = pairs[a][b][0] + pairs[a][b][1]
                total = total + (OWN * both if a == b else both)
            others = [diffs[b] for b in range(3) if b != a]
            up, down = shifts[a](others[0] + others[1])
            out.append(KEEP * w[a] + p[a] + q * (total + MIX * (up - down)))
        return tuple(out)

    return lax.fori_loop(0, COARSE - 1, step, tuple(p))


def second_kernel(
    every,
    y3,
    tail2,
    pq,
    tail_pq,
    f,
    out,
    sum_out,
    x3,
    x4,
    tail3,
    tail4,
    w_ref,
    n_ref,
    edges,
    out_sem,
):
    gx, gx_n, _ = position(GX)
    gy, gy_n, _ = position("gy")
    gz, gz_n, _ = position(GZ)
    me = (gx * gy_n + gy) * gz_n + gz
    lane = lanes_of((8, 128))
    row8 = rows_of((8, 128))
    cells = jnp.transpose(every[...])
    load = [cells[8 * c : 8 * c + 8] for c in range(3)]
    mean = cells[24:32] * (1.0 / BLOCK**3)
    load_sum = jnp.sum(cells[32:40])
    w = coarse_solve(load, mean, gx_n, gy_n, gz_n)
    n = gx_n * gy_n * gz_n
    centre = n // 2
    own_cells = (lane // BLOCK == row8).astype(F32)
    line = lane[:1]
    cell_of = ((7, -1), (0, 0), (7, 0), (0, 1))
    spans = ((4, 4), (8, 16), (24, 4))
    x_cell_in = (gx > 0, True, gx < gx_n - 1)
    y_cell_in = (gy > 0, True, gy < gy_n - 1)
    for c in range(3):
        turned = pltpu.roll(w[c], (centre + n - me) % n, 1)

        def column(dx, dy):
            return centre + (dx - 1) * gy_n * gz_n + (dy - 1) * gz_n

        for dy in range(3):
            first, size = spans[dy]
            for dx in range(3):
                j = column(dx, dy)
                main = jnp.sum(turned[:, j : j + 1] * own_cells, axis=0, keepdims=True)
                main = jnp.where(x_cell_in[dx] & y_cell_in[dy], main, 0.0)
                for k in range(3 * dx, 3 * dx + 3):
                    w_ref[k, c, pl.ds(first, size), :] = jnp.broadcast_to(main, (size, 128))
            for page in range(4):
                k, dz = cell_of[page]
                here = [
                    jnp.broadcast_to(
                        turned[k : k + 1, column(dx, dy) + dz : column(dx, dy) + dz + 1], (1, 128)
                    )
                    for dx in range(3)
                ]
                value = jnp.where(
                    line < W * W, here[0], jnp.where(line < W * (W + 16), here[1], here[2])
                )
                rows = pl.ds(first, size)
                inside = tail_pq[page, 3, rows, :] > 0.0
                tail3[page, c, rows, :] = tail2[page, c, rows, :] + jnp.where(inside, value, 0.0)

    tail_sweep(tail3, tail4, tail_pq)
    for k in range(1, 8):
        for row in GROUPS:
            sums, _ = neighbour_sum(w_ref, None, k, row, lane)
            for c in range(3):
                n_ref[k, c, pl.ds(row, 8), :] = sums[c]
    ends = (lane < 2) | (lane >= 126)
    for row in GROUPS:
        for c in range(3):
            rows = pl.ds(row, 8)
            edges[c, rows, :] = jnp.where(
                lane % W < 2, tail4[1, c, rows, :], pltpu.roll(tail4[2, c, rows, :], 128 - W, 1)
            )

    def correct(i, carry):
        k = jnp.minimum(i - 1, W) + jnp.maximum(i - W - 14, 0)
        for row in GROUPS:
            rows = pl.ds(row, 8)
            q = pq[i, 3, rows, :]
            for c in range(3):
                edge = pltpu.roll(edges[c, rows, :], 128 - W * i, 1)
                value = y3[i, c, rows, :] + KEEP * w_ref[k, c, rows, :] + q * n_ref[k, c, rows, :]
                x4[i, c, rows, :] = jnp.where(ends, edge, value)
        return carry

    planes(2, NP - 2, correct)
    tail_sweep(tail4, tail3, tail_pq, edges, True)
    sweep(x4, x3, pq, edges, 3, NP - 3)
    copies = [
        pltpu.make_async_copy(
            x3.at[pl.ds(W, 16), c, pl.ds(8, 16), :], out.at[c], out_sem.at[c]
        )
        for c in range(3)
    ]
    for copy in copies:
        copy.start()
    edges_only(tail3, edges)

    def residual(i, total):
        for row in OWN_GROUPS:
            sums, v = neighbour_sum(x3, edges, i, row, lane)
            rows = pl.ds(row - 8, 8)
            g = stiffness_of(f[3, i - W, rows, :])
            d = (g * DIAG + MASS_TERM) * (1.0 / RELAXATION)
            q = pq[i, 3, pl.ds(row, 8), :]
            for c in range(3):
                p = pq[i, c, pl.ds(row, 8), :]
                r = d * ((p - RELAXATION * v[c]) + q * sums[c])
                total += r * r
        return total

    total = jnp.sum(planes(W, W + 16, residual, jnp.zeros((8, 128), F32)))
    both = jnp.where(line == 0, load_sum * (1.0 / n), total)
    sum_out[...] = jnp.broadcast_to(both, sum_out.shape)
    for copy in copies:
        copy.wait()


def swaps(far_send, near_send, axis):
    count = lax.axis_size(axis)
    near = [(i, i ^ 1) for i in range(count)]
    far = [(i, ((i ^ 1) + (2 if i % 2 else -2)) % count) for i in range(count)]
    return lax.ppermute(far_send, axis, far), lax.ppermute(near_send, axis, near)


VMEM = pl.BlockSpec(memory_space=pltpu.VMEM)
SMEM = pl.BlockSpec(memory_space=pltpu.SMEM)
HBM = pl.BlockSpec(memory_space=pltpu.HBM)


def call(kernel, shapes, arguments, mib, scratch=(), source=VMEM, target=VMEM):
    shapes = [jax.ShapeDtypeStruct(shape, F32) for shape in shapes]
    return pl.pallas_call(
        kernel,
        out_shape=tuple(shapes),
        in_specs=[source] * len(arguments),
        out_specs=target if isinstance(target, tuple) else (target,) * len(shapes),
        scratch_shapes=[pltpu.VMEM(s, F32) if isinstance(s, tuple) else s for s in scratch],
        compiler_params=pltpu.CompilerParams(vmem_limit_bytes=mib << 20),
    )(*arguments)


def norms_kernel(count, parts, out):
    root = jnp.sqrt(jnp.sum(parts[...], axis=0, keepdims=True) * (1.0 / count))
    out[0] = root[0, 0]
    out[1] = root[0, 1]


def on_device(right_side, damage):
    n = lax.axis_size(ALL)
    slab = (4, W, 16, 128)
    f, *x_sends = call(
        x_pack_kernel,
        ((4, 16, 16, 128), slab, slab),
        tuple(pltpu.with_memory_space_constraint(x, pltpu.HBM) for x in (right_side, damage)),
        8,
        (
            pltpu.VMEM((16, 16, 128), jnp.int32),
            pltpu.SemaphoreType.DMA(()),
            pltpu.SemaphoreType.DMA(()),
        ),
        source=HBM,
    )
    x_pieces = swaps(*x_sends, GX)
    slab = (4, NP // 2, 8, 128)
    y_sends = call(y_pack_kernel, (slab, slab), (f, *x_pieces), 8)
    y_pieces = swaps(*y_sends, "gy")
    pieces = (f, *x_pieces, *y_pieces)
    side = (4, NP, 128)
    own_side = (4, 16, 128)
    own_sends = call(z_pack_own_kernel, (own_side, own_side), (f, *x_pieces), 8)
    z_sends = call(z_pack_kernel, (side, side), (*y_pieces, *own_sends), 8)
    z_pieces = swaps(*z_sends, GZ)
    field = (NP, 4, ROWS, 128)
    tails = (4, 4, ROWS, 128)
    edges = (3, ROWS, 128)
    pq, y3, columns = call(main_kernel, (field, field, (8, 128)), pieces, 12, (field,))
    tail, tail_pq, sums = call(
        first_kernel, (tails, tails, (n, 128)), (columns, *z_sends, *z_pieces), 8
    )
    every = lax.all_to_all(sums, ALL, 0, 0, tiled=True)
    displacement, partial_sums = call(
        second_kernel,
        (right_side.shape, (n, 128)),
        (every, y3, tail, pq, tail_pq, f),
        20,
        (
            *(field, field, tails, tails),
            *((9, 4, ROWS, 128), (9, 4, ROWS, 128), edges),
            pltpu.SemaphoreType.DMA((3,)),
        ),
        target=(HBM, VMEM),
    )
    partial_sums = lax.all_to_all(partial_sums, ALL, 0, 0, tiled=True)
    (norms,) = call(
        functools.partial(norms_kernel, right_side.size * n), ((2,),), (partial_sums,), 2, target=SMEM
    )
    return (displacement, norms)


def solution(mesh):
    torus = Mesh(mesh.devices.reshape(4, 2, mesh.shape["gy"], 2, 4), ALL)
    placed = (P(None, GX, "gy", GZ), P(GX, "gy", GZ))
    return jax.shard_map(
        on_device,
        mesh=torus,
        in_specs=placed,
        out_specs=(P(None, GX, "gy", GZ), P()),
        check_vma=False,
    )
```

```python
import functools

import jax
import jax.numpy as jnp
from jax import lax
from jax.experimental import pallas as pl
from jax.experimental.pallas import tpu as pltpu
from jax.sharding import Mesh
from jax.sharding import PartitionSpec as P

BLOCK = 16
COARSE = 8
GX = ("gx_0", "gx_1")
GZ = ("gz_0", "gz_1")
ALL = ("gx_0", "gx_1", "gy", "gz_0", "gz_1")

FLOOR_STIFFNESS = 0.05
MASS_TERM = 0.001
COUPLING = 2.5
RELAXATION = 0.6

W = 4
NP = 16 + 2 * W
ROWS = 40
GROUPS = (4, 12, 20)
OWN_GROUPS = (8, 16)
DIAG = 6.0 + 2.0 * COUPLING
OWN = 1.0 + COUPLING
MIX = 0.25 * COUPLING
KEEP = 1.0 - RELAXATION
F32 = jnp.float32


def lanes_of(shape):
    return lax.broadcasted_iota(jnp.int32, shape, 1)


def rows_of(shape):
    return lax.broadcasted_iota(jnp.int32, shape, 0)


def stiffness_of(damage):
    level = damage.astype(F32) / 15.0
    return (1.0 - level) ** 2 * (1.0 - FLOOR_STIFFNESS) + FLOOR_STIFFNESS


def position(axis):
    at = lax.axis_index(axis)
    return at, lax.axis_size(axis), at % 2


def pick(odd, when_odd, when_even):
    return jnp.where(odd, when_odd, when_even)


def tail_parts(tail, row, page):
    v = [tail[page, c, pl.ds(row, 8), :] for c in range(3)]
    yp = [tail[page, c, pl.ds(row + 1, 8), :] for c in range(3)]
    ym = [tail[page, c, pl.ds(row - 1, 8), :] for c in range(3)]
    xp = [pltpu.roll(v[c], 128 - W, 1) for c in range(3)]
    xm = [pltpu.roll(v[c], W, 1) for c in range(3)]
    zx = MIX * (xp[2] - xm[2])
    zy = MIX * (yp[2] - ym[2])
    zz = MIX * ((xp[0] - xm[0]) + (yp[1] - ym[1]))
    own = OWN * v[2]
    ups = (v[0] + zx, v[1] + zy, own + zz)
    downs = (v[0] - zx, v[1] - zy, own - zz)
    return ups, downs, v, xp, xm, yp, ym


def tail_sums(source, row, low):
    lane = lanes_of((8, 128))
    parts = [tail_parts(source, row, page) for page in (low, low + 1)]
    (up_a, down_a), (up_b, down_b) = (part[:2] for part in parts)
    first = lane % W == 0
    last = lane % W == W - 1
    beside_z = (
        [
            jnp.where(last, pltpu.roll(up_b[c], W - 1, 1), pltpu.roll(up_a[c], 127, 1))
            + pltpu.roll(down_a[c], 1, 1)
            for c in range(3)
        ],
        [
            jnp.where(first, pltpu.roll(down_a[c], 129 - W, 1), pltpu.roll(down_b[c], 1, 1))
            + pltpu.roll(up_b[c], 127, 1)
            for c in range(3)
        ],
    )
    sums = []
    for t in range(2):
        _, _, v, xp, xm, yp, ym = parts[t]
        dy0 = MIX * (yp[0] - ym[0])
        dy1 = MIX * (yp[1] - ym[1])
        mix_x = pltpu.roll(dy1, 128 - W, 1) - pltpu.roll(dy1, W, 1)
        mix_y = pltpu.roll(dy0, 128 - W, 1) - pltpu.roll(dy0, W, 1)
        rest = (
            OWN * (xp[0] + xm[0]) + (yp[0] + ym[0]) + mix_x,
            OWN * (yp[1] + ym[1]) + (xp[1] + xm[1]) + mix_y,
            (xp[2] + xm[2]) + (yp[2] + ym[2]),
        )
        sums.append([rest[c] + beside_z[t][c] for c in range(3)])
    return sums, [part[2] for part in parts], up_b, down_a


def put_edges(edges, row, ups, downs):
    last = lanes_of((8, 128)) % W == W - 1
    for c in range(3):
        edges[c, pl.ds(row, 8), :] = jnp.where(
            last, pltpu.roll(ups[c], 127, 1), pltpu.roll(downs[c], 129 - W, 1)
        )


def tail_sweep(source, target, pq, edges=None, outer_only=False):
    for row in GROUPS:
        kept = {}
        for low in (0, 2):
            sums, v, up_b, down_a = tail_sums(source, row, low)
            kept[low] = up_b, down_a
            for t in range(2):
                if outer_only and low + t in (1, 2):
                    continue
                q = pq[low + t, 3, pl.ds(row, 8), :]
                for c in range(3):
                    p = pq[low + t, c, pl.ds(row, 8), :]
                    target[low + t, c, pl.ds(row, 8), :] = KEEP * v[t][c] + p + q * sums[t][c]
        if edges is not None:
            put_edges(edges, row, kept[2][0], kept[0][1])


def edges_only(source, edges):
    for row in OWN_GROUPS:
        put_edges(
            edges, row, tail_parts(source, row, 3)[0], tail_parts(source, row, 0)[1]
        )


def neighbour_sum(ref, edges, i, row, lane):
    def at(c, dx, dy):
        return ref[i + dx, c, pl.ds(row + dy, 8), :]

    v = [at(c, 0, 0) for c in range(3)]
    xp = [at(c, 1, 0) for c in range(3)]
    xm = [at(c, -1, 0) for c in range(3)]
    yp = [at(c, 0, 1) for c in range(3)]
    ym = [at(c, 0, -1) for c in range(3)]
    zx = MIX * (xp[2] - xm[2])
    zy = MIX * (yp[2] - ym[2])
    zz = MIX * ((xp[0] - xm[0]) + (yp[1] - ym[1]))
    own = OWN * v[2]
    ups = (v[0] + zx, v[1] + zy, own + zz)
    downs = (v[0] - zx, v[1] - zy, own - zz)
    mix_x = (at(1, 1, 1) - at(1, 1, -1)) - (at(1, -1, 1) - at(1, -1, -1))
    mix_y = (at(0, 1, 1) - at(0, 1, -1)) - (at(0, -1, 1) - at(0, -1, -1))
    rest = (
        OWN * (xp[0] + xm[0]) + (yp[0] + ym[0]) + MIX * mix_x,
        OWN * (yp[1] + ym[1]) + (xp[1] + xm[1]) + MIX * mix_y,
        (xp[2] + xm[2]) + (yp[2] + ym[2]),
    )
    sums = []
    for c in range(3):
        up, down = pltpu.roll(ups[c], 127, 1), pltpu.roll(downs[c], 1, 1)
        if edges is not None:
            edge = pltpu.roll(edges[c, pl.ds(row, 8), :], 128 - W * i, 1)
            up = jnp.where(lane == 127, edge, up)
            down = jnp.where(lane == 0, edge, down)
        sums.append(rest[c] + (up + down))
    return sums, v


def planes(first, last, body, carry=0, step=4):
    whole = first + (last - first) // step * step

    def some(k, carry):
        for j in range(step):
            carry = body(first + step * k + j, carry)
        return carry

    carry = lax.fori_loop(0, (last - first) // step, some, carry)
    for i in range(whole, last):
        carry = body(i, carry)
    return carry


def sweep(source, target, pq, edges, first, last, step=4):
    lane = lanes_of((8, 128))

    def plane(i, carry):
        for row in GROUPS:
            sums, v = neighbour_sum(source, edges, i, row, lane)
            q = pq[i, 3, pl.ds(row, 8), :]
            for c in range(3):
                p = pq[i, c, pl.ds(row, 8), :]
                target[i, c, pl.ds(row, 8), :] = KEEP * v[c] + p + q * sums[c]
        return carry

    planes(first, last, plane, step=step)


def x_pack_kernel(load, damage, f_out, far_out, near_out, level, load_sem, level_sem):
    odd = position(GX)[2] == 1
    load_copy = pltpu.make_async_copy(load, f_out.at[pl.ds(0, 3)], load_sem)
    level_copy = pltpu.make_async_copy(damage, level, level_sem)
    load_copy.start()
    level_copy.start()
    level_copy.wait()
    f_out[3] = level[...].astype(F32)
    load_copy.wait()
    for c in range(4):
        for i in range(W):
            low, high = f_out[c, i], f_out[c, i + 16 - W]
            far_out[c, i] = pick(odd, high, low)
            near_out[c, i] = pick(odd, low, high)


def y_pack_kernel(f, xfar, xnear, far_out, near_out):
    odd_x, odd_y = position(GX)[2] == 1, position("gy")[2] == 1
    upper = rows_of((8, 128)) < 4

    def tile(c, i, k):
        rows = pl.ds(8 * k, 8)
        if i < W:
            return pick(odd_x, xnear[c, i, rows, :], xfar[c, i, rows, :])
        if i >= W + 16:
            return pick(odd_x, xfar[c, i - W - 16, rows, :], xnear[c, i - W - 16, rows, :])
        return f[c, i - W, rows, :]

    for c in range(4):
        for j in range(NP // 2):
            a, b = 2 * j, 2 * j + 1
            low = jnp.where(upper, tile(c, a, 0), pltpu.roll(tile(c, b, 0), 4, 0))
            high = jnp.where(upper, pltpu.roll(tile(c, a, 1), 4, 0), tile(c, b, 1))
            far_out[c, j] = pick(odd_y, high, low)
            near_out[c, j] = pick(odd_y, low, high)


def put_z_pack(values, rows, odd_z, far_out, near_out):
    lane = lanes_of((8, 128))
    for c in range(4):
        far = jnp.zeros((8, 128), F32)
        near = far
        for i in range(NP):
            value = values(c, i)
            here = (lane >= W * i) & (lane < W * i + W)
            far = jnp.where(here, pltpu.roll(value, W * i + W * odd_z, 1), far)
            near = jnp.where(here, pltpu.roll(value, W * i + W * (1 - odd_z), 1), near)
        far_out[c, rows, :] = far
        near_out[c, rows, :] = near


def z_pack_own_kernel(f, xfar, xnear, far_out, near_out):
    odd_x = position(GX)[2] == 1
    for k in range(2):
        rows = pl.ds(8 * k, 8)

        def values(c, i):
            if i < W:
                return pick(odd_x, xnear[c, i, rows, :], xfar[c, i, rows, :])
            if i >= W + 16:
                j = i - W - 16
                return pick(odd_x, xfar[c, j, rows, :], xnear[c, j, rows, :])
            return f[c, i - W, rows, :]

        put_z_pack(values, rows, position(GZ)[2], far_out, near_out)


def z_pack_kernel(yfar, ynear, far_own, near_own, far_out, near_out):
    odd_y = position("gy")[2] == 1
    upper = rows_of((8, 128)) < 4
    for c in range(4):
        far_out[c, pl.ds(0, 16), :] = far_own[c]
        near_out[c, pl.ds(0, 16), :] = near_own[c]

    def values(c, i):
        low = pick(odd_y, ynear[c, i // 2], yfar[c, i // 2])
        high = pick(odd_y, yfar[c, i // 2], ynear[c, i // 2])
        if i % 2:
            return jnp.where(upper, pltpu.roll(low, 4, 0), high)
        return jnp.where(upper, low, pltpu.roll(high, 4, 0))

    put_z_pack(values, pl.ds(16, 8), position(GZ)[2], far_out, near_out)


def main_kernel(f, xfar, xnear, yfar, ynear, pq, y3, by_cell, x2):
    gx, gx_n, odd_x = position(GX)
    gy, gy_n, odd_y = position("gy")
    odd_x, odd_y = odd_x == 1, odd_y == 1

    def x_inside(i):
        x = gx * 16 + i - W
        return (x >= 0) & (x < gx_n * 16)

    def values(parts, inside):
        g = stiffness_of(parts[3])
        scale = RELAXATION / (g * DIAG + MASS_TERM)
        out = [part * scale for part in parts[:3]] + [g * scale]
        return [jnp.where(inside, value, 0.0) for value in out]

    def fill(i, parts):
        for c, value in enumerate(values(parts, x_inside(i))):
            pq[i, c, pl.ds(8, 16), :] = value

    def own(i, carry):
        fill(i, [f[c, i - W] for c in range(4)])
        return carry

    lax.fori_loop(W, W + 16, own, 0)

    def beside_x(i, carry):
        fill(i, [pick(odd_x, xnear[c, i], xfar[c, i]) for c in range(4)])
        fill(i + W + 16, [pick(odd_x, xfar[c, i], xnear[c, i]) for c in range(4)])
        return carry

    lax.fori_loop(0, W, beside_x, 0)
    second = (rows_of((8, 128)) >= 4).astype(jnp.int32)
    low_in, high_in = gy > 0, gy < gy_n - 1

    def beside_y(j, carry):
        inside = x_inside(2 * j + second)
        low = values([pick(odd_y, ynear[c, j], yfar[c, j]) for c in range(4)], inside & low_in)
        high = values([pick(odd_y, yfar[c, j], ynear[c, j]) for c in range(4)], inside & high_in)
        for c in range(4):
            for t in range(2):
                pq[2 * j + t, c, pl.ds(4, 4), :] = low[c][4 * t : 4 * t + 4]
                pq[2 * j + t, c, pl.ds(24, 4), :] = high[c][4 * t : 4 * t + 4]
        return carry

    lax.fori_loop(0, NP // 2, beside_y, 0)
    sweep(pq, x2, pq, None, 1, NP - 1)
    lane = lanes_of((8, 128))
    row8 = rows_of((8, 128))

    def residual(i, carry):
        totals = list(carry)
        for row in OWN_GROUPS:
            sums, v = neighbour_sum(x2, None, i, row, lane)
            rows = pl.ds(row - 8, 8)
            g = stiffness_of(f[3, i - W, rows, :])
            d = g * DIAG + MASS_TERM
            for c in range(3):
                load = f[c, i - W, rows, :]
                totals[c] += (load - d * v[c]) + g * sums[c]
                totals[4] += load * load
            totals[3] += g
        return tuple(totals)

    zero = jnp.zeros((8, 128), F32)
    totals = planes(W, W + 16, residual, (zero,) * 5)
    stacked = zero
    inner = (lane >= 2) & (lane < 126)
    for c in range(5):
        total = jnp.where(inner, totals[c], 0.0) if c < 3 else totals[c]
        stacked = jnp.where(row8 == c, jnp.sum(total, axis=0, keepdims=True), stacked)
    big = (128, 128)
    gather = (rows_of(big) // BLOCK == lanes_of(big) % 8).astype(F32)
    by_cell[...] = jnp.dot(
        stacked, gather, precision=lax.Precision.HIGHEST, preferred_element_type=F32
    )
    sweep(x2, y3, pq, None, 2, NP - 2)


def first_kernel(by_cell, zfar_own, znear_own, zfar, znear, tail, tail_pq, sums_out):
    lane = lanes_of((8, 128))
    row8 = rows_of((8, 128))
    gx, gx_n, _ = position(GX)
    gy, gy_n, _ = position("gy")
    gz, gz_n, odd_z = position(GZ)
    odd_z = odd_z == 1
    x = gx * 16 + lane // W - W
    x_in = (x >= 0) & (x < gx_n * 16)
    y_in = ((row8 >= 4) | (gy > 0)) & ((row8 < 4) | (gy < gy_n - 1))
    z_in = (gz > 0, True, True, gz < gz_n - 1)
    sides = (
        (znear, zfar),
        (znear_own, zfar_own),
        (zfar_own, znear_own),
        (zfar, znear),
    )

    def part(page, c, k):
        when_odd, when_even = sides[page]
        rows = pl.ds(8 * k, 8)
        return pick(odd_z, when_odd[c, rows, :], when_even[c, rows, :])

    for page in range(4):
        for k in range(3):
            g = stiffness_of(part(page, 3, k))
            scale = RELAXATION / (g * DIAG + MASS_TERM)
            inside = x_in
            if page in (0, 3):
                inside = inside & z_in[page]
            if k == 2:
                inside = inside & y_in
            for c in range(4):
                value = jnp.where(inside, (part(page, c, k) if c < 3 else g) * scale, 0.0)
                if k < 2:
                    tail_pq[page, c, pl.ds(8 + 8 * k, 8), :] = value
                else:
                    tail_pq[page, c, pl.ds(4, 4), :] = value[:4]
                    tail_pq[page, c, pl.ds(24, 4), :] = value[4:]
    tail_sweep(tail_pq, tail, tail_pq)
    zero = jnp.zeros((8, 128), F32)
    ends = zero
    for side in range(2):
        page = 1 + side
        here = (lane % W < 2) if side == 0 else (lane % W >= 2)
        totals = [zero] * 3
        for row in OWN_GROUPS:
            sums, v, _, _ = tail_sums(tail, row, 2 * side)
            k = row // 8 - 1
            g = stiffness_of(part(page, 3, k))
            d = g * DIAG + MASS_TERM
            for c in range(3):
                totals[c] += (part(page, c, k) - d * v[1 - side][c]) + g * sums[1 - side][c]
        for c in range(3):
            total = jnp.sum(jnp.where(here, totals[c], 0.0), axis=0, keepdims=True)
            ends = jnp.where(row8 == 3 * side + c, total, ends)
    ends = jnp.where((lane >= W * W) & (lane < W * (W + 16)), ends, 0.0)
    by_end = jnp.sum(ends, axis=1, keepdims=True)
    low_end = (lane % 8 == 0) & (lane // 8 == row8) & (row8 < 3)
    high_end = (lane % 8 == 7) & (lane // 8 + 3 == row8) & (row8 < 6)
    slot = jnp.where(lane // 8 == row8, by_cell[...], 0.0) + jnp.where(
        low_end | high_end, by_end, 0.0
    )
    sums_out[...] = jnp.broadcast_to(jnp.sum(slot, axis=0, keepdims=True), sums_out.shape)


def coarse_solve(load, mean, gx_n, gy_n, gz_n):
    shape = load[0].shape
    n = shape[1]
    lane = lanes_of(shape)
    row = rows_of(shape)
    sx, sy = gy_n * gz_n, gz_n
    x_at, y_at, z_at = lane // sx, lane // sy % gy_n, lane % gz_n

    def shift(v, step, at, count):
        up = jnp.where(at < count - 1, pltpu.roll(v, n - step, 1), 0.0)
        down = jnp.where(at > 0, pltpu.roll(v, step, 1), 0.0)
        return up, down

    def shift_z(v):
        up = pltpu.roll(v, 7, 0)
        down = pltpu.roll(v, 1, 0)
        next_up = jnp.where(z_at < gz_n - 1, pltpu.roll(up, n - 1, 1), 0.0)
        next_down = jnp.where(z_at > 0, pltpu.roll(down, 1, 1), 0.0)
        return jnp.where(row == 7, next_up, up), jnp.where(row == 0, next_down, down)

    shifts = (
        lambda v: shift(v, sx, x_at, gx_n),
        lambda v: shift(v, sy, y_at, gy_n),
        shift_z,
    )
    coefficient = BLOCK**2 * mean
    scale = RELAXATION / (coefficient * DIAG + BLOCK**3 * MASS_TERM)
    p = [scale * value for value in load]
    q = scale * coefficient

    def step(_, w):
        pairs = [[shifts[b](w[a]) for b in range(3)] for a in range(3)]
        diffs = [pairs[a][a][0] - pairs[a][a][1] for a in range(3)]
        out = []
        for a in range(3):
            total = 0.0
            for b in range(3):
                both = pairs[a][b][0] + pairs[a][b][1]
                total = total + (OWN * both if a == b else both)
            others = [diffs[b] for b in range(3) if b != a]
            up, down = shifts[a](others[0] + others[1])
            out.append(KEEP * w[a] + p[a] + q * (total + MIX * (up - down)))
        return tuple(out)

    return lax.fori_loop(0, COARSE - 1, step, tuple(p))


def second_kernel(
    every,
    y3,
    tail2,
    pq,
    tail_pq,
    f,
    out,
    sum_out,
    load_out,
    x3,
    x4,
    tail3,
    tail4,
    w_ref,
    n_ref,
    edges,
    out_sem,
):
    gx, gx_n, _ = position(GX)
    gy, gy_n, _ = position("gy")
    gz, gz_n, _ = position(GZ)
    me = (gx * gy_n + gy) * gz_n + gz
    lane = lanes_of((8, 128))
    row8 = rows_of((8, 128))
    cells = jnp.transpose(every[...])
    load = [cells[8 * c : 8 * c + 8] for c in range(3)]
    mean = cells[24:32] * (1.0 / BLOCK**3)
    load_out[...] = cells[32:40]
    w = coarse_solve(load, mean, gx_n, gy_n, gz_n)
    n = gx_n * gy_n * gz_n
    centre = n // 2
    own_cells = (lane // BLOCK == row8).astype(F32)
    line = lane[:1]
    cell_of = ((7, -1), (0, 0), (7, 0), (0, 1))
    spans = ((4, 4), (8, 16), (24, 4))
    x_cell_in = (gx > 0, True, gx < gx_n - 1)
    y_cell_in = (gy > 0, True, gy < gy_n - 1)
    for c in range(3):
        turned = pltpu.roll(w[c], (centre + n - me) % n, 1)

        def column(dx, dy):
            return centre + (dx - 1) * gy_n * gz_n + (dy - 1) * gz_n

        for dy in range(3):
            first, size = spans[dy]
            for dx in range(3):
                j = column(dx, dy)
                main = jnp.sum(turned[:, j : j + 1] * own_cells, axis=0, keepdims=True)
                main = jnp.where(x_cell_in[dx] & y_cell_in[dy], main, 0.0)
                for k in range(3 * dx, 3 * dx + 3):
                    w_ref[k, c, pl.ds(first, size), :] = jnp.broadcast_to(main, (size, 128))
            for page in range(4):
                k, dz = cell_of[page]
                here = [
                    jnp.broadcast_to(
                        turned[k : k + 1, column(dx, dy) + dz : column(dx, dy) + dz + 1], (1, 128)
                    )
                    for dx in range(3)
                ]
                value = jnp.where(
                    line < W * W, here[0], jnp.where(line < W * (W + 16), here[1], here[2])
                )
                rows = pl.ds(first, size)
                inside = tail_pq[page, 3, rows, :] > 0.0
                tail3[page, c, rows, :] = tail2[page, c, rows, :] + jnp.where(inside, value, 0.0)

    tail_sweep(tail3, tail4, tail_pq)
    for k in range(1, 8):
        for row in GROUPS:
            sums, _ = neighbour_sum(w_ref, None, k, row, lane)
            for c in range(3):
                n_ref[k, c, pl.ds(row, 8), :] = sums[c]
    ends = (lane < 2) | (lane >= 126)
    for row in GROUPS:
        for c in range(3):
            rows = pl.ds(row, 8)
            edges[c, rows, :] = jnp.where(
                lane % W < 2, tail4[1, c, rows, :], pltpu.roll(tail4[2, c, rows, :], 128 - W, 1)
            )

    def correct(i, carry):
        k = jnp.minimum(i - 1, W) + jnp.maximum(i - W - 14, 0)
        for row in GROUPS:
            rows = pl.ds(row, 8)
            q = pq[i, 3, rows, :]
            for c in range(3):
                edge = pltpu.roll(edges[c, rows, :], 128 - W * i, 1)
                value = y3[i, c, rows, :] + KEEP * w_ref[k, c, rows, :] + q * n_ref[k, c, rows, :]
                x4[i, c, rows, :] = jnp.where(ends, edge, value)
        return carry

    planes(2, NP - 2, correct)
    tail_sweep(tail4, tail3, tail_pq, edges, True)
    sweep(x4, x3, pq, edges, 3, NP - 3, 6)
    copies = [
        pltpu.make_async_copy(
            x3.at[pl.ds(W, 16), c, pl.ds(8, 16), :], out.at[c], out_sem.at[c]
        )
        for c in range(3)
    ]
    for copy in copies:
        copy.start()
    edges_only(tail3, edges)

    def residual(i, total):
        for row in OWN_GROUPS:
            sums, v = neighbour_sum(x3, edges, i, row, lane)
            rows = pl.ds(row - 8, 8)
            g = stiffness_of(f[3, i - W, rows, :])
            d = (g * DIAG + MASS_TERM) * (1.0 / RELAXATION)
            q = pq[i, 3, pl.ds(row, 8), :]
            for c in range(3):
                p = pq[i, c, pl.ds(row, 8), :]
                r = d * ((p - RELAXATION * v[c]) + q * sums[c])
                total += r * r
        return total

    total = planes(W, W + 16, residual, jnp.zeros((8, 128), F32))
    sum_out[...] = jnp.broadcast_to(jnp.sum(total, axis=0, keepdims=True), sum_out.shape)
    for copy in copies:
        copy.wait()


def swaps(far_send, near_send, axis):
    count = lax.axis_size(axis)
    near = [(i, i ^ 1) for i in range(count)]
    far = [(i, ((i ^ 1) + (2 if i % 2 else -2)) % count) for i in range(count)]
    return lax.ppermute(far_send, axis, far), lax.ppermute(near_send, axis, near)


VMEM = pl.BlockSpec(memory_space=pltpu.VMEM)
SMEM = pl.BlockSpec(memory_space=pltpu.SMEM)
HBM = pl.BlockSpec(memory_space=pltpu.HBM)


def call(kernel, shapes, arguments, mib, scratch=(), source=VMEM, target=VMEM):
    shapes = [jax.ShapeDtypeStruct(shape, F32) for shape in shapes]
    return pl.pallas_call(
        kernel,
        out_shape=tuple(shapes),
        in_specs=[source] * len(arguments),
        out_specs=target if isinstance(target, tuple) else (target,) * len(shapes),
        scratch_shapes=[pltpu.VMEM(s, F32) if isinstance(s, tuple) else s for s in scratch],
        compiler_params=pltpu.CompilerParams(vmem_limit_bytes=mib << 20),
    )(*arguments)


def norms_kernel(count, load_parts, residual_parts, out):
    for k, parts in enumerate((load_parts, residual_parts)):
        line = jnp.sum(parts[...], axis=0, keepdims=True)
        total = jnp.sum(line, axis=1, keepdims=True)
        out[k] = jnp.sqrt(total * (1.0 / count))[0, 0]


def on_device(right_side, damage):
    n = lax.axis_size(ALL)
    slab = (4, W, 16, 128)
    f, *x_sends = call(
        x_pack_kernel,
        ((4, 16, 16, 128), slab, slab),
        tuple(pltpu.with_memory_space_constraint(x, pltpu.HBM) for x in (right_side, damage)),
        8,
        (
            pltpu.VMEM((16, 16, 128), jnp.int32),
            pltpu.SemaphoreType.DMA(()),
            pltpu.SemaphoreType.DMA(()),
        ),
        source=HBM,
    )
    x_pieces = swaps(*x_sends, GX)
    slab = (4, NP // 2, 8, 128)
    y_sends = call(y_pack_kernel, (slab, slab), (f, *x_pieces), 8)
    y_pieces = swaps(*y_sends, "gy")
    pieces = (f, *x_pieces, *y_pieces)
    side = (4, NP, 128)
    own_side = (4, 16, 128)
    own_sends = call(z_pack_own_kernel, (own_side, own_side), (f, *x_pieces), 8)
    z_sends = call(z_pack_kernel, (side, side), (*y_pieces, *own_sends), 8)
    z_pieces = swaps(*z_sends, GZ)
    field = (NP, 4, ROWS, 128)
    tails = (4, 4, ROWS, 128)
    edges = (4, ROWS, 128)
    pq, y3, by_cell = call(main_kernel, (field, field, (8, 128)), pieces, 12, (field,))
    tail, tail_pq, sums = call(
        first_kernel, (tails, tails, (n, 128)), (by_cell, *z_sends, *z_pieces), 8
    )
    every = lax.all_to_all(sums, ALL, 0, 0, tiled=True)
    displacement, partial_sums, load_sums = call(
        second_kernel,
        (right_side.shape, (n, 128), (8, n)),
        (every, y3, tail, pq, tail_pq, f),
        20,
        (
            *(field, field, tails, tails),
            *((12, 4, ROWS, 128), (12, 4, ROWS, 128), edges),
            pltpu.SemaphoreType.DMA((3,)),
        ),
        target=(HBM, VMEM, VMEM),
    )
    partial_sums = lax.all_to_all(partial_sums, ALL, 0, 0, tiled=True)
    (norms,) = call(
        functools.partial(norms_kernel, right_side.size * n), ((2,),), (load_sums, partial_sums), 2, target=SMEM
    )
    return (displacement, norms)


def solution(mesh):
    torus = Mesh(mesh.devices.reshape(4, 2, mesh.shape["gy"], 2, 4), ALL)
    placed = (P(None, GX, "gy", GZ), P(GX, "gy", GZ))
    return jax.shard_map(
        on_device,
        mesh=torus,
        in_specs=placed,
        out_specs=(P(None, GX, "gy", GZ), P()),
        check_vma=False,
    )
```

```python
import functools

import jax
import jax.numpy as jnp
from jax import lax
from jax.experimental import pallas as pl
from jax.experimental.pallas import tpu as pltpu
from jax.sharding import Mesh
from jax.sharding import PartitionSpec as P

BLOCK = 16
COARSE = 8
GX = ("gx_0", "gx_1")
GZ = ("gz_0", "gz_1")
ALL = ("gx_0", "gx_1", "gy", "gz_0", "gz_1")

FLOOR_STIFFNESS = 0.05
MASS_TERM = 0.001
COUPLING = 2.5
RELAXATION = 0.6

W = 4
NP = 16 + 2 * W
ROWS = 40
GROUPS = (4, 12, 20)
OWN_GROUPS = (8, 16)
DIAG = 6.0 + 2.0 * COUPLING
OWN = 1.0 + COUPLING
MIX = 0.25 * COUPLING
KEEP = 1.0 - RELAXATION
F32 = jnp.float32


def lanes_of(shape):
    return lax.broadcasted_iota(jnp.int32, shape, 1)


def rows_of(shape):
    return lax.broadcasted_iota(jnp.int32, shape, 0)


def stiffness_of(damage):
    level = damage.astype(F32) / 15.0
    return (1.0 - level) ** 2 * (1.0 - FLOOR_STIFFNESS) + FLOOR_STIFFNESS


def position(axis):
    at = lax.axis_index(axis)
    return at, lax.axis_size(axis), at % 2


def pick(odd, when_odd, when_even):
    return jnp.where(odd, when_odd, when_even)


def tail_parts(tail, row, page):
    v = [tail[page, c, pl.ds(row, 8), :] for c in range(3)]
    yp = [tail[page, c, pl.ds(row + 1, 8), :] for c in range(3)]
    ym = [tail[page, c, pl.ds(row - 1, 8), :] for c in range(3)]
    xp = [pltpu.roll(v[c], 128 - W, 1) for c in range(3)]
    xm = [pltpu.roll(v[c], W, 1) for c in range(3)]
    zx = MIX * (xp[2] - xm[2])
    zy = MIX * (yp[2] - ym[2])
    zz = MIX * ((xp[0] - xm[0]) + (yp[1] - ym[1]))
    own = OWN * v[2]
    ups = (v[0] + zx, v[1] + zy, own + zz)
    downs = (v[0] - zx, v[1] - zy, own - zz)
    return ups, downs, v, xp, xm, yp, ym


def tail_sums(source, row, low):
    lane = lanes_of((8, 128))
    parts = [tail_parts(source, row, page) for page in (low, low + 1)]
    (up_a, down_a), (up_b, down_b) = (part[:2] for part in parts)
    first = lane % W == 0
    last = lane % W == W - 1
    beside_z = (
        [
            jnp.where(last, pltpu.roll(up_b[c], W - 1, 1), pltpu.roll(up_a[c], 127, 1))
            + pltpu.roll(down_a[c], 1, 1)
            for c in range(3)
        ],
        [
            jnp.where(first, pltpu.roll(down_a[c], 129 - W, 1), pltpu.roll(down_b[c], 1, 1))
            + pltpu.roll(up_b[c], 127, 1)
            for c in range(3)
        ],
    )
    sums = []
    for t in range(2):
        _, _, v, xp, xm, yp, ym = parts[t]
        dy0 = MIX * (yp[0] - ym[0])
        dy1 = MIX * (yp[1] - ym[1])
        mix_x = pltpu.roll(dy1, 128 - W, 1) - pltpu.roll(dy1, W, 1)
        mix_y = pltpu.roll(dy0, 128 - W, 1) - pltpu.roll(dy0, W, 1)
        rest = (
            OWN * (xp[0] + xm[0]) + (yp[0] + ym[0]) + mix_x,
            OWN * (yp[1] + ym[1]) + (xp[1] + xm[1]) + mix_y,
            (xp[2] + xm[2]) + (yp[2] + ym[2]),
        )
        sums.append([rest[c] + beside_z[t][c] for c in range(3)])
    return sums, [part[2] for part in parts], up_b, down_a


def put_edges(edges, row, ups, downs):
    last = lanes_of((8, 128)) % W == W - 1
    for c in range(3):
        edges[c, pl.ds(row, 8), :] = jnp.where(
            last, pltpu.roll(ups[c], 127, 1), pltpu.roll(downs[c], 129 - W, 1)
        )


def tail_sweep(source, target, pq, edges=None, outer_only=False):
    for row in GROUPS:
        kept = {}
        for low in (0, 2):
            sums, v, up_b, down_a = tail_sums(source, row, low)
            kept[low] = up_b, down_a
            for t in range(2):
                if outer_only and low + t in (1, 2):
                    continue
                q = pq[low + t, 3, pl.ds(row, 8), :]
                for c in range(3):
                    p = pq[low + t, c, pl.ds(row, 8), :]
                    target[low + t, c, pl.ds(row, 8), :] = KEEP * v[t][c] + p + q * sums[t][c]
        if edges is not None:
            put_edges(edges, row, kept[2][0], kept[0][1])


def edges_only(source, edges):
    for row in OWN_GROUPS:
        put_edges(
            edges, row, tail_parts(source, row, 3)[0], tail_parts(source, row, 0)[1]
        )


def neighbour_sum(ref, edges, i, row, lane):
    def at(c, dx, dy):
        return ref[i + dx, c, pl.ds(row + dy, 8), :]

    v = [at(c, 0, 0) for c in range(3)]
    xp = [at(c, 1, 0) for c in range(3)]
    xm = [at(c, -1, 0) for c in range(3)]
    yp = [at(c, 0, 1) for c in range(3)]
    ym = [at(c, 0, -1) for c in range(3)]
    zx = MIX * (xp[2] - xm[2])
    zy = MIX * (yp[2] - ym[2])
    zz = MIX * ((xp[0] - xm[0]) + (yp[1] - ym[1]))
    own = OWN * v[2]
    ups = (v[0] + zx, v[1] + zy, own + zz)
    downs = (v[0] - zx, v[1] - zy, own - zz)
    mix_x = (at(1, 1, 1) - at(1, 1, -1)) - (at(1, -1, 1) - at(1, -1, -1))
    mix_y = (at(0, 1, 1) - at(0, 1, -1)) - (at(0, -1, 1) - at(0, -1, -1))
    rest = (
        OWN * (xp[0] + xm[0]) + (yp[0] + ym[0]) + MIX * mix_x,
        OWN * (yp[1] + ym[1]) + (xp[1] + xm[1]) + MIX * mix_y,
        (xp[2] + xm[2]) + (yp[2] + ym[2]),
    )
    sums = []
    for c in range(3):
        up, down = pltpu.roll(ups[c], 127, 1), pltpu.roll(downs[c], 1, 1)
        if edges is not None:
            edge = pltpu.roll(edges[c, pl.ds(row, 8), :], 128 - W * i, 1)
            up = jnp.where(lane == 127, edge, up)
            down = jnp.where(lane == 0, edge, down)
        sums.append(rest[c] + (up + down))
    return sums, v


def planes(first, last, body, carry=0, step=4):
    whole = first + (last - first) // step * step

    def some(k, carry):
        for j in range(step):
            carry = body(first + step * k + j, carry)
        return carry

    carry = lax.fori_loop(0, (last - first) // step, some, carry)
    for i in range(whole, last):
        carry = body(i, carry)
    return carry


def sweep(source, target, pq, edges, first, last, step=4):
    lane = lanes_of((8, 128))

    def plane(i, carry):
        for row in GROUPS:
            sums, v = neighbour_sum(source, edges, i, row, lane)
            q = pq[i, 3, pl.ds(row, 8), :]
            for c in range(3):
                p = pq[i, c, pl.ds(row, 8), :]
                target[i, c, pl.ds(row, 8), :] = KEEP * v[c] + p + q * sums[c]
        return carry

    planes(first, last, plane, step=step)


def x_pack_kernel(load, damage, f_out, far_out, near_out, level, load_sem, level_sem):
    odd = position(GX)[2] == 1
    load_copy = pltpu.make_async_copy(load, f_out.at[pl.ds(0, 3)], load_sem)
    level_copy = pltpu.make_async_copy(damage, level, level_sem)
    load_copy.start()
    level_copy.start()
    level_copy.wait()
    f_out[3] = level[...].astype(F32)
    load_copy.wait()
    for c in range(4):
        for i in range(W):
            low, high = f_out[c, i], f_out[c, i + 16 - W]
            far_out[c, i] = pick(odd, high, low)
            near_out[c, i] = pick(odd, low, high)


def y_pack_kernel(f, xfar, xnear, far_out, near_out):
    odd_x, odd_y = position(GX)[2] == 1, position("gy")[2] == 1
    upper = rows_of((8, 128)) < 4

    def tile(c, i, k):
        rows = pl.ds(8 * k, 8)
        if i < W:
            return pick(odd_x, xnear[c, i, rows, :], xfar[c, i, rows, :])
        if i >= W + 16:
            return pick(odd_x, xfar[c, i - W - 16, rows, :], xnear[c, i - W - 16, rows, :])
        return f[c, i - W, rows, :]

    for c in range(4):
        for j in range(NP // 2):
            a, b = 2 * j, 2 * j + 1
            low = jnp.where(upper, tile(c, a, 0), pltpu.roll(tile(c, b, 0), 4, 0))
            high = jnp.where(upper, pltpu.roll(tile(c, a, 1), 4, 0), tile(c, b, 1))
            far_out[c, j] = pick(odd_y, high, low)
            near_out[c, j] = pick(odd_y, low, high)


def put_z_pack(values, rows, odd_z, far_out, near_out):
    lane = lanes_of((8, 128))
    for c in range(4):
        far = jnp.zeros((8, 128), F32)
        near = far
        for i in range(NP):
            value = values(c, i)
            here = (lane >= W * i) & (lane < W * i + W)
            far = jnp.where(here, pltpu.roll(value, W * i + W * odd_z, 1), far)
            near = jnp.where(here, pltpu.roll(value, W * i + W * (1 - odd_z), 1), near)
        far_out[c, rows, :] = far
        near_out[c, rows, :] = near


def z_pack_own_kernel(f, xfar, xnear, far_out, near_out):
    odd_x = position(GX)[2] == 1
    for k in range(2):
        rows = pl.ds(8 * k, 8)

        def values(c, i):
            if i < W:
                return pick(odd_x, xnear[c, i, rows, :], xfar[c, i, rows, :])
            if i >= W + 16:
                j = i - W - 16
                return pick(odd_x, xfar[c, j, rows, :], xnear[c, j, rows, :])
            return f[c, i - W, rows, :]

        put_z_pack(values, rows, position(GZ)[2], far_out, near_out)


def z_pack_kernel(yfar, ynear, far_own, near_own, far_out, near_out):
    odd_y = position("gy")[2] == 1
    upper = rows_of((8, 128)) < 4
    for c in range(4):
        far_out[c, pl.ds(0, 16), :] = far_own[c]
        near_out[c, pl.ds(0, 16), :] = near_own[c]

    def values(c, i):
        low = pick(odd_y, ynear[c, i // 2], yfar[c, i // 2])
        high = pick(odd_y, yfar[c, i // 2], ynear[c, i // 2])
        if i % 2:
            return jnp.where(upper, pltpu.roll(low, 4, 0), high)
        return jnp.where(upper, low, pltpu.roll(high, 4, 0))

    put_z_pack(values, pl.ds(16, 8), position(GZ)[2], far_out, near_out)


def main_kernel(f, xfar, xnear, yfar, ynear, pq, y3, by_cell, x2):
    gx, gx_n, odd_x = position(GX)
    gy, gy_n, odd_y = position("gy")
    odd_x, odd_y = odd_x == 1, odd_y == 1

    def x_inside(i):
        x = gx * 16 + i - W
        return (x >= 0) & (x < gx_n * 16)

    def values(parts, inside):
        g = stiffness_of(parts[3])
        scale = RELAXATION / (g * DIAG + MASS_TERM)
        out = [part * scale for part in parts[:3]] + [g * scale]
        return [jnp.where(inside, value, 0.0) for value in out]

    def fill(i, parts):
        for c, value in enumerate(values(parts, x_inside(i))):
            pq[i, c, pl.ds(8, 16), :] = value

    def own(i, carry):
        fill(i, [f[c, i - W] for c in range(4)])
        return carry

    lax.fori_loop(W, W + 16, own, 0)

    def beside_x(i, carry):
        fill(i, [pick(odd_x, xnear[c, i], xfar[c, i]) for c in range(4)])
        fill(i + W + 16, [pick(odd_x, xfar[c, i], xnear[c, i]) for c in range(4)])
        return carry

    lax.fori_loop(0, W, beside_x, 0)
    second = (rows_of((8, 128)) >= 4).astype(jnp.int32)
    low_in, high_in = gy > 0, gy < gy_n - 1

    def beside_y(j, carry):
        inside = x_inside(2 * j + second)
        low = values([pick(odd_y, ynear[c, j], yfar[c, j]) for c in range(4)], inside & low_in)
        high = values([pick(odd_y, yfar[c, j], ynear[c, j]) for c in range(4)], inside & high_in)
        for c in range(4):
            for t in range(2):
                pq[2 * j + t, c, pl.ds(4, 4), :] = low[c][4 * t : 4 * t + 4]
                pq[2 * j + t, c, pl.ds(24, 4), :] = high[c][4 * t : 4 * t + 4]
        return carry

    lax.fori_loop(0, NP // 2, beside_y, 0)
    sweep(pq, x2, pq, None, 1, NP - 1)
    lane = lanes_of((8, 128))
    row8 = rows_of((8, 128))

    def residual(i, carry):
        totals = list(carry)
        for row in OWN_GROUPS:
            sums, v = neighbour_sum(x2, None, i, row, lane)
            rows = pl.ds(row - 8, 8)
            g = stiffness_of(f[3, i - W, rows, :])
            d = g * DIAG + MASS_TERM
            for c in range(3):
                load = f[c, i - W, rows, :]
                totals[c] += (load - d * v[c]) + g * sums[c]
                totals[4] += load * load
            totals[3] += g
        return tuple(totals)

    zero = jnp.zeros((8, 128), F32)
    totals = planes(W, W + 16, residual, (zero,) * 5)
    stacked = zero
    inner = (lane >= 2) & (lane < 126)
    for c in range(5):
        total = jnp.where(inner, totals[c], 0.0) if c < 3 else totals[c]
        stacked = jnp.where(row8 == c, jnp.sum(total, axis=0, keepdims=True), stacked)
    big = (128, 128)
    gather = (rows_of(big) // BLOCK == lanes_of(big) % 8).astype(F32)
    by_cell[...] = jnp.dot(
        stacked, gather, precision=lax.Precision.HIGHEST, preferred_element_type=F32
    )
    sweep(x2, y3, pq, None, 2, NP - 2)


def first_kernel(by_cell, zfar_own, znear_own, zfar, znear, tail, tail_pq, sums_out):
    lane = lanes_of((8, 128))
    row8 = rows_of((8, 128))
    gx, gx_n, _ = position(GX)
    gy, gy_n, _ = position("gy")
    gz, gz_n, odd_z = position(GZ)
    odd_z = odd_z == 1
    x = gx * 16 + lane // W - W
    x_in = (x >= 0) & (x < gx_n * 16)
    y_in = ((row8 >= 4) | (gy > 0)) & ((row8 < 4) | (gy < gy_n - 1))
    z_in = (gz > 0, True, True, gz < gz_n - 1)
    sides = (
        (znear, zfar),
        (znear_own, zfar_own),
        (zfar_own, znear_own),
        (zfar, znear),
    )

    def part(page, c, k):
        when_odd, when_even = sides[page]
        rows = pl.ds(8 * k, 8)
        return pick(odd_z, when_odd[c, rows, :], when_even[c, rows, :])

    for page in range(4):
        for k in range(3):
            g = stiffness_of(part(page, 3, k))
            scale = RELAXATION / (g * DIAG + MASS_TERM)
            inside = x_in
            if page in (0, 3):
                inside = inside & z_in[page]
            if k == 2:
                inside = inside & y_in
            for c in range(4):
                value = jnp.where(inside, (part(page, c, k) if c < 3 else g) * scale, 0.0)
                if k < 2:
                    tail_pq[page, c, pl.ds(8 + 8 * k, 8), :] = value
                else:
                    tail_pq[page, c, pl.ds(4, 4), :] = value[:4]
                    tail_pq[page, c, pl.ds(24, 4), :] = value[4:]
    tail_sweep(tail_pq, tail, tail_pq)
    zero = jnp.zeros((8, 128), F32)
    ends = zero
    for side in range(2):
        page = 1 + side
        here = (lane % W < 2) if side == 0 else (lane % W >= 2)
        totals = [zero] * 3
        for row in OWN_GROUPS:
            sums, v, _, _ = tail_sums(tail, row, 2 * side)
            k = row // 8 - 1
            g = stiffness_of(part(page, 3, k))
            d = g * DIAG + MASS_TERM
            for c in range(3):
                totals[c] += (part(page, c, k) - d * v[1 - side][c]) + g * sums[1 - side][c]
        for c in range(3):
            total = jnp.sum(jnp.where(here, totals[c], 0.0), axis=0, keepdims=True)
            ends = jnp.where(row8 == 3 * side + c, total, ends)
    ends = jnp.where((lane >= W * W) & (lane < W * (W + 16)), ends, 0.0)
    by_end = jnp.sum(ends, axis=1, keepdims=True)
    low_end = (lane % 8 == 0) & (lane // 8 == row8) & (row8 < 3)
    high_end = (lane % 8 == 7) & (lane // 8 + 3 == row8) & (row8 < 6)
    slot = jnp.where(lane // 8 == row8, by_cell[...], 0.0) + jnp.where(
        low_end | high_end, by_end, 0.0
    )
    sums_out[...] = jnp.broadcast_to(jnp.sum(slot, axis=0, keepdims=True), sums_out.shape)


def coarse_solve(load, mean, gx_n, gy_n, gz_n):
    shape = load[0].shape
    n = shape[1]
    lane = lanes_of(shape)
    row = rows_of(shape)
    sx, sy = gy_n * gz_n, gz_n
    x_at, y_at, z_at = lane // sx, lane // sy % gy_n, lane % gz_n

    def shift(v, step, at, count):
        up = jnp.where(at < count - 1, pltpu.roll(v, n - step, 1), 0.0)
        down = jnp.where(at > 0, pltpu.roll(v, step, 1), 0.0)
        return up, down

    def shift_z(v):
        up = pltpu.roll(v, 7, 0)
        down = pltpu.roll(v, 1, 0)
        next_up = jnp.where(z_at < gz_n - 1, pltpu.roll(up, n - 1, 1), 0.0)
        next_down = jnp.where(z_at > 0, pltpu.roll(down, 1, 1), 0.0)
        return jnp.where(row == 7, next_up, up), jnp.where(row == 0, next_down, down)

    shifts = (
        lambda v: shift(v, sx, x_at, gx_n),
        lambda v: shift(v, sy, y_at, gy_n),
        shift_z,
    )
    coefficient = BLOCK**2 * mean
    scale = RELAXATION / (coefficient * DIAG + BLOCK**3 * MASS_TERM)
    p = [scale * value for value in load]
    q = scale * coefficient

    def step(_, w):
        pairs = [[shifts[b](w[a]) for b in range(3)] for a in range(3)]
        diffs = [pairs[a][a][0] - pairs[a][a][1] for a in range(3)]
        out = []
        for a in range(3):
            total = 0.0
            for b in range(3):
                both = pairs[a][b][0] + pairs[a][b][1]
                total = total + (OWN * both if a == b else both)
            others = [diffs[b] for b in range(3) if b != a]
            up, down = shifts[a](others[0] + others[1])
            out.append(KEEP * w[a] + p[a] + q * (total + MIX * (up - down)))
        return tuple(out)

    w = tuple(p)
    for k in range(COARSE - 1):
        w = step(k, w)
    return w


def second_kernel(
    every,
    y3,
    tail2,
    pq,
    tail_pq,
    f,
    out,
    sum_out,
    load_out,
    x3,
    x4,
    tail3,
    tail4,
    w_ref,
    n_ref,
    edges,
    out_sem,
):
    gx, gx_n, _ = position(GX)
    gy, gy_n, _ = position("gy")
    gz, gz_n, _ = position(GZ)
    me = (gx * gy_n + gy) * gz_n + gz
    lane = lanes_of((8, 128))
    row8 = rows_of((8, 128))
    cells = jnp.transpose(every[...])
    load = [cells[8 * c : 8 * c + 8] for c in range(3)]
    mean = cells[24:32] * (1.0 / BLOCK**3)
    load_out[...] = cells[32:40]
    w = coarse_solve(load, mean, gx_n, gy_n, gz_n)
    n = gx_n * gy_n * gz_n
    centre = n // 2
    own_cells = (lane // BLOCK == row8).astype(F32)
    line = lane[:1]
    cell_of = ((7, -1), (0, 0), (7, 0), (0, 1))
    spans = ((4, 4), (8, 16), (24, 4))
    x_cell_in = (gx > 0, True, gx < gx_n - 1)
    y_cell_in = (gy > 0, True, gy < gy_n - 1)
    for c in range(3):
        turned = pltpu.roll(w[c], (centre + n - me) % n, 1)

        def column(dx, dy):
            return centre + (dx - 1) * gy_n * gz_n + (dy - 1) * gz_n

        for dy in range(3):
            first, size = spans[dy]
            for dx in range(3):
                j = column(dx, dy)
                main = jnp.sum(turned[:, j : j + 1] * own_cells, axis=0, keepdims=True)
                main = jnp.where(x_cell_in[dx] & y_cell_in[dy], main, 0.0)
                for k in range(3 * dx, 3 * dx + 3):
                    w_ref[k, c, pl.ds(first, size), :] = jnp.broadcast_to(main, (size, 128))
            for page in range(4):
                k, dz = cell_of[page]
                here = [
                    jnp.broadcast_to(
                        turned[k : k + 1, column(dx, dy) + dz : column(dx, dy) + dz + 1], (1, 128)
                    )
                    for dx in range(3)
                ]
                value = jnp.where(
                    line < W * W, here[0], jnp.where(line < W * (W + 16), here[1], here[2])
                )
                rows = pl.ds(first, size)
                inside = tail_pq[page, 3, rows, :] > 0.0
                tail3[page, c, rows, :] = tail2[page, c, rows, :] + jnp.where(inside, value, 0.0)

    tail_sweep(tail3, tail4, tail_pq)
    for k in range(1, 8):
        for row in GROUPS:
            sums, _ = neighbour_sum(w_ref, None, k, row, lane)
            for c in range(3):
                n_ref[k, c, pl.ds(row, 8), :] = sums[c]
    ends = (lane < 2) | (lane >= 126)
    for row in GROUPS:
        for c in range(3):
            rows = pl.ds(row, 8)
            edges[c, rows, :] = jnp.where(
                lane % W < 2, tail4[1, c, rows, :], pltpu.roll(tail4[2, c, rows, :], 128 - W, 1)
            )

    def correct(i, carry):
        k = jnp.minimum(i - 1, W) + jnp.maximum(i - W - 14, 0)
        for row in GROUPS:
            rows = pl.ds(row, 8)
            q = pq[i, 3, rows, :]
            for c in range(3):
                edge = pltpu.roll(edges[c, rows, :], 128 - W * i, 1)
                value = y3[i, c, rows, :] + KEEP * w_ref[k, c, rows, :] + q * n_ref[k, c, rows, :]
                x4[i, c, rows, :] = jnp.where(ends, edge, value)
        return carry

    planes(2, NP - 2, correct)
    tail_sweep(tail4, tail3, tail_pq, edges, True)
    sweep(x4, x3, pq, edges, 3, NP - 3, 6)
    copies = [
        pltpu.make_async_copy(
            x3.at[pl.ds(W, 16), c, pl.ds(8, 16), :], out.at[c], out_sem.at[c]
        )
        for c in range(3)
    ]
    for copy in copies:
        copy.start()
    edges_only(tail3, edges)

    def residual(i, total):
        for row in OWN_GROUPS:
            sums, v = neighbour_sum(x3, edges, i, row, lane)
            rows = pl.ds(row - 8, 8)
            g = stiffness_of(f[3, i - W, rows, :])
            d = (g * DIAG + MASS_TERM) * (1.0 / RELAXATION)
            q = pq[i, 3, pl.ds(row, 8), :]
            for c in range(3):
                p = pq[i, c, pl.ds(row, 8), :]
                r = d * ((p - RELAXATION * v[c]) + q * sums[c])
                total += r * r
        return total

    total = planes(W, W + 16, residual, jnp.zeros((8, 128), F32), step=8)
    sum_out[...] = jnp.broadcast_to(jnp.sum(total, axis=0, keepdims=True), sum_out.shape)
    for copy in copies:
        copy.wait()


def swaps(far_send, near_send, axis):
    count = lax.axis_size(axis)
    near = [(i, i ^ 1) for i in range(count)]
    far = [(i, ((i ^ 1) + (2 if i % 2 else -2)) % count) for i in range(count)]
    return lax.ppermute(far_send, axis, far), lax.ppermute(near_send, axis, near)


VMEM = pl.BlockSpec(memory_space=pltpu.VMEM)
SMEM = pl.BlockSpec(memory_space=pltpu.SMEM)
HBM = pl.BlockSpec(memory_space=pltpu.HBM)


def call(kernel, shapes, arguments, mib, scratch=(), source=VMEM, target=VMEM):
    shapes = [jax.ShapeDtypeStruct(shape, F32) for shape in shapes]
    return pl.pallas_call(
        kernel,
        out_shape=tuple(shapes),
        in_specs=[source] * len(arguments),
        out_specs=target if isinstance(target, tuple) else (target,) * len(shapes),
        scratch_shapes=[pltpu.VMEM(s, F32) if isinstance(s, tuple) else s for s in scratch],
        compiler_params=pltpu.CompilerParams(vmem_limit_bytes=mib << 20),
    )(*arguments)


def norms_kernel(count, load_parts, residual_parts, out):
    for k, parts in enumerate((load_parts, residual_parts)):
        line = jnp.sum(parts[...], axis=0, keepdims=True)
        total = jnp.sum(line, axis=1, keepdims=True)
        out[k] = jnp.sqrt(total * (1.0 / count))[0, 0]


def on_device(right_side, damage):
    n = lax.axis_size(ALL)
    slab = (4, W, 16, 128)
    f, *x_sends = call(
        x_pack_kernel,
        ((4, 16, 16, 128), slab, slab),
        tuple(pltpu.with_memory_space_constraint(x, pltpu.HBM) for x in (right_side, damage)),
        8,
        (
            pltpu.VMEM((16, 16, 128), jnp.int32),
            pltpu.SemaphoreType.DMA(()),
            pltpu.SemaphoreType.DMA(()),
        ),
        source=HBM,
    )
    x_pieces = swaps(*x_sends, GX)
    slab = (4, NP // 2, 8, 128)
    y_sends = call(y_pack_kernel, (slab, slab), (f, *x_pieces), 8)
    y_pieces = swaps(*y_sends, "gy")
    pieces = (f, *x_pieces, *y_pieces)
    side = (4, NP, 128)
    own_side = (4, 16, 128)
    own_sends = call(z_pack_own_kernel, (own_side, own_side), (f, *x_pieces), 8)
    z_sends = call(z_pack_kernel, (side, side), (*y_pieces, *own_sends), 8)
    z_pieces = swaps(*z_sends, GZ)
    field = (NP, 4, ROWS, 128)
    tails = (4, 4, ROWS, 128)
    edges = (4, ROWS, 128)
    pq, y3, by_cell = call(main_kernel, (field, field, (8, 128)), pieces, 12, (field,))
    tail, tail_pq, sums = call(
        first_kernel, (tails, tails, (n, 128)), (by_cell, *z_sends, *z_pieces), 8
    )
    every = lax.all_to_all(sums, ALL, 0, 0, tiled=True)
    displacement, partial_sums, load_sums = call(
        second_kernel,
        (right_side.shape, (n, 128), (8, n)),
        (every, y3, tail, pq, tail_pq, f),
        20,
        (
            *(field, field, tails, tails),
            *((12, 4, ROWS, 128), (12, 4, ROWS, 128), edges),
            pltpu.SemaphoreType.DMA((3,)),
        ),
        target=(HBM, VMEM, VMEM),
    )
    partial_sums = lax.all_to_all(partial_sums, ALL, 0, 0, tiled=True)
    (norms,) = call(
        functools.partial(norms_kernel, right_side.size * n), ((2,),), (load_sums, partial_sums), 2, target=SMEM
    )
    return (displacement, norms)


def solution(mesh):
    torus = Mesh(mesh.devices.reshape(4, 2, mesh.shape["gy"], 2, 4), ALL)
    placed = (P(None, GX, "gy", GZ), P(GX, "gy", GZ))
    return jax.shard_map(
        on_device,
        mesh=torus,
        in_specs=placed,
        out_specs=(P(None, GX, "gy", GZ), P()),
        check_vma=False,
    )
```

```python
import functools

import jax
import jax.numpy as jnp
from jax import lax
from jax.experimental import pallas as pl
from jax.experimental.pallas import tpu as pltpu
from jax.sharding import Mesh
from jax.sharding import PartitionSpec as P

BLOCK = 16
COARSE = 8
GX = ("gx_0", "gx_1")
GZ = ("gz_0", "gz_1")
ALL = ("gx_0", "gx_1", "gy", "gz_0", "gz_1")

FLOOR_STIFFNESS = 0.05
MASS_TERM = 0.001
COUPLING = 2.5
RELAXATION = 0.6

W = 4
NP = 16 + 2 * W
ROWS = 40
GROUPS = (4, 12, 20)
OWN_GROUPS = (8, 16)
DIAG = 6.0 + 2.0 * COUPLING
OWN = 1.0 + COUPLING
MIX = 0.25 * COUPLING
KEEP = 1.0 - RELAXATION
F32 = jnp.float32


def lanes_of(shape):
    return lax.broadcasted_iota(jnp.int32, shape, 1)


def rows_of(shape):
    return lax.broadcasted_iota(jnp.int32, shape, 0)


def stiffness_of(damage):
    level = damage.astype(F32) / 15.0
    return (1.0 - level) ** 2 * (1.0 - FLOOR_STIFFNESS) + FLOOR_STIFFNESS


def position(axis):
    at = lax.axis_index(axis)
    return at, lax.axis_size(axis), at % 2


def pick(odd, when_odd, when_even):
    return jnp.where(odd, when_odd, when_even)


def tail_parts(tail, row, page):
    v = [tail[page, c, pl.ds(row, 8), :] for c in range(3)]
    yp = [tail[page, c, pl.ds(row + 1, 8), :] for c in range(3)]
    ym = [tail[page, c, pl.ds(row - 1, 8), :] for c in range(3)]
    xp = [pltpu.roll(v[c], 128 - W, 1) for c in range(3)]
    xm = [pltpu.roll(v[c], W, 1) for c in range(3)]
    zx = MIX * (xp[2] - xm[2])
    zy = MIX * (yp[2] - ym[2])
    zz = MIX * ((xp[0] - xm[0]) + (yp[1] - ym[1]))
    own = OWN * v[2]
    ups = (v[0] + zx, v[1] + zy, own + zz)
    downs = (v[0] - zx, v[1] - zy, own - zz)
    return ups, downs, v, xp, xm, yp, ym


def tail_sums(source, row, low):
    lane = lanes_of((8, 128))
    parts = [tail_parts(source, row, page) for page in (low, low + 1)]
    (up_a, down_a), (up_b, down_b) = (part[:2] for part in parts)
    first = lane % W == 0
    last = lane % W == W - 1
    beside_z = (
        [
            jnp.where(last, pltpu.roll(up_b[c], W - 1, 1), pltpu.roll(up_a[c], 127, 1))
            + pltpu.roll(down_a[c], 1, 1)
            for c in range(3)
        ],
        [
            jnp.where(first, pltpu.roll(down_a[c], 129 - W, 1), pltpu.roll(down_b[c], 1, 1))
            + pltpu.roll(up_b[c], 127, 1)
            for c in range(3)
        ],
    )
    sums = []
    for t in range(2):
        _, _, v, xp, xm, yp, ym = parts[t]
        dy0 = MIX * (yp[0] - ym[0])
        dy1 = MIX * (yp[1] - ym[1])
        mix_x = pltpu.roll(dy1, 128 - W, 1) - pltpu.roll(dy1, W, 1)
        mix_y = pltpu.roll(dy0, 128 - W, 1) - pltpu.roll(dy0, W, 1)
        rest = (
            OWN * (xp[0] + xm[0]) + (yp[0] + ym[0]) + mix_x,
            OWN * (yp[1] + ym[1]) + (xp[1] + xm[1]) + mix_y,
            (xp[2] + xm[2]) + (yp[2] + ym[2]),
        )
        sums.append([rest[c] + beside_z[t][c] for c in range(3)])
    return sums, [part[2] for part in parts], up_b, down_a


def put_edges(edges, row, ups, downs):
    last = lanes_of((8, 128)) % W == W - 1
    for c in range(3):
        edges[c, pl.ds(row, 8), :] = jnp.where(
            last, pltpu.roll(ups[c], 127, 1), pltpu.roll(downs[c], 129 - W, 1)
        )


def tail_sweep(source, target, pq, edges=None, outer_only=False):
    for row in GROUPS:
        kept = {}
        for low in (0, 2):
            sums, v, up_b, down_a = tail_sums(source, row, low)
            kept[low] = up_b, down_a
            for t in range(2):
                if outer_only and low + t in (1, 2):
                    continue
                q = pq[low + t, 3, pl.ds(row, 8), :]
                for c in range(3):
                    p = pq[low + t, c, pl.ds(row, 8), :]
                    target[low + t, c, pl.ds(row, 8), :] = KEEP * v[t][c] + p + q * sums[t][c]
        if edges is not None:
            put_edges(edges, row, kept[2][0], kept[0][1])


def edges_only(source, edges):
    for row in OWN_GROUPS:
        put_edges(
            edges, row, tail_parts(source, row, 3)[0], tail_parts(source, row, 0)[1]
        )


def neighbour_sum(ref, edges, i, row, lane):
    def at(c, dx, dy):
        return ref[i + dx, c, pl.ds(row + dy, 8), :]

    v = [at(c, 0, 0) for c in range(3)]
    xp = [at(c, 1, 0) for c in range(3)]
    xm = [at(c, -1, 0) for c in range(3)]
    yp = [at(c, 0, 1) for c in range(3)]
    ym = [at(c, 0, -1) for c in range(3)]
    zx = MIX * (xp[2] - xm[2])
    zy = MIX * (yp[2] - ym[2])
    zz = MIX * ((xp[0] - xm[0]) + (yp[1] - ym[1]))
    own = OWN * v[2]
    ups = (v[0] + zx, v[1] + zy, own + zz)
    downs = (v[0] - zx, v[1] - zy, own - zz)
    mix_x = (at(1, 1, 1) - at(1, 1, -1)) - (at(1, -1, 1) - at(1, -1, -1))
    mix_y = (at(0, 1, 1) - at(0, 1, -1)) - (at(0, -1, 1) - at(0, -1, -1))
    rest = (
        OWN * (xp[0] + xm[0]) + (yp[0] + ym[0]) + MIX * mix_x,
        OWN * (yp[1] + ym[1]) + (xp[1] + xm[1]) + MIX * mix_y,
        (xp[2] + xm[2]) + (yp[2] + ym[2]),
    )
    sums = []
    for c in range(3):
        up, down = pltpu.roll(ups[c], 127, 1), pltpu.roll(downs[c], 1, 1)
        if edges is not None:
            edge = pltpu.roll(edges[c, pl.ds(row, 8), :], 128 - W * i, 1)
            up = jnp.where(lane == 127, edge, up)
            down = jnp.where(lane == 0, edge, down)
        sums.append(rest[c] + (up + down))
    return sums, v


def planes(first, last, body, carry=0, step=4):
    whole = first + (last - first) // step * step

    def some(k, carry):
        for j in range(step):
            carry = body(first + step * k + j, carry)
        return carry

    carry = lax.fori_loop(0, (last - first) // step, some, carry)
    for i in range(whole, last):
        carry = body(i, carry)
    return carry


def sweep(source, target, pq, edges, first, last, step=4):
    lane = lanes_of((8, 128))

    def plane(i, carry):
        for row in GROUPS:
            sums, v = neighbour_sum(source, edges, i, row, lane)
            q = pq[i, 3, pl.ds(row, 8), :]
            for c in range(3):
                p = pq[i, c, pl.ds(row, 8), :]
                target[i, c, pl.ds(row, 8), :] = KEEP * v[c] + p + q * sums[c]
        return carry

    planes(first, last, plane, step=step)


def x_pack_kernel(load, damage, f_out, far_out, near_out, level, load_sem, level_sem):
    odd = position(GX)[2] == 1
    load_copy = pltpu.make_async_copy(load, f_out.at[pl.ds(0, 3)], load_sem)
    level_copy = pltpu.make_async_copy(damage, level, level_sem)
    load_copy.start()
    level_copy.start()
    level_copy.wait()
    f_out[3] = level[...].astype(F32)
    load_copy.wait()
    for c in range(4):
        for i in range(W):
            low, high = f_out[c, i], f_out[c, i + 16 - W]
            far_out[c, i] = pick(odd, high, low)
            near_out[c, i] = pick(odd, low, high)


def y_pack_kernel(f, xfar, xnear, far_out, near_out):
    odd_x, odd_y = position(GX)[2] == 1, position("gy")[2] == 1
    upper = rows_of((8, 128)) < 4

    def tile(c, i, k):
        rows = pl.ds(8 * k, 8)
        if i < W:
            return pick(odd_x, xnear[c, i, rows, :], xfar[c, i, rows, :])
        if i >= W + 16:
            return pick(odd_x, xfar[c, i - W - 16, rows, :], xnear[c, i - W - 16, rows, :])
        return f[c, i - W, rows, :]

    for c in range(4):
        for j in range(NP // 2):
            a, b = 2 * j, 2 * j + 1
            low = jnp.where(upper, tile(c, a, 0), pltpu.roll(tile(c, b, 0), 4, 0))
            high = jnp.where(upper, pltpu.roll(tile(c, a, 1), 4, 0), tile(c, b, 1))
            far_out[c, j] = pick(odd_y, high, low)
            near_out[c, j] = pick(odd_y, low, high)


def put_z_pack(values, rows, odd_z, far_out, near_out):
    lane = lanes_of((8, 128))
    for c in range(4):
        far = jnp.zeros((8, 128), F32)
        near = far
        for i in range(NP):
            value = values(c, i)
            here = (lane >= W * i) & (lane < W * i + W)
            far = jnp.where(here, pltpu.roll(value, W * i + W * odd_z, 1), far)
            near = jnp.where(here, pltpu.roll(value, W * i + W * (1 - odd_z), 1), near)
        far_out[c, rows, :] = far
        near_out[c, rows, :] = near


def z_pack_own_kernel(f, xfar, xnear, far_out, near_out):
    odd_x = position(GX)[2] == 1
    for k in range(2):
        rows = pl.ds(8 * k, 8)

        def values(c, i):
            if i < W:
                return pick(odd_x, xnear[c, i, rows, :], xfar[c, i, rows, :])
            if i >= W + 16:
                j = i - W - 16
                return pick(odd_x, xfar[c, j, rows, :], xnear[c, j, rows, :])
            return f[c, i - W, rows, :]

        put_z_pack(values, rows, position(GZ)[2], far_out, near_out)


def z_pack_kernel(yfar, ynear, far_own, near_own, far_out, near_out):
    odd_y = position("gy")[2] == 1
    upper = rows_of((8, 128)) < 4
    for c in range(4):
        far_out[c, pl.ds(0, 16), :] = far_own[c]
        near_out[c, pl.ds(0, 16), :] = near_own[c]

    def values(c, i):
        low = pick(odd_y, ynear[c, i // 2], yfar[c, i // 2])
        high = pick(odd_y, yfar[c, i // 2], ynear[c, i // 2])
        if i % 2:
            return jnp.where(upper, pltpu.roll(low, 4, 0), high)
        return jnp.where(upper, low, pltpu.roll(high, 4, 0))

    put_z_pack(values, pl.ds(16, 8), position(GZ)[2], far_out, near_out)


def main_kernel(f, xfar, xnear, yfar, ynear, pq, y3, by_cell, x2):
    gx, gx_n, odd_x = position(GX)
    gy, gy_n, odd_y = position("gy")
    odd_x, odd_y = odd_x == 1, odd_y == 1

    def x_inside(i):
        x = gx * 16 + i - W
        return (x >= 0) & (x < gx_n * 16)

    def values(parts, inside):
        g = stiffness_of(parts[3])
        scale = RELAXATION / (g * DIAG + MASS_TERM)
        out = [part * scale for part in parts[:3]] + [g * scale]
        return [jnp.where(inside, value, 0.0) for value in out]

    def fill(i, parts):
        for c, value in enumerate(values(parts, x_inside(i))):
            pq[i, c, pl.ds(8, 16), :] = value

    def own(i, carry):
        fill(i, [f[c, i - W] for c in range(4)])
        return carry

    lax.fori_loop(W, W + 16, own, 0)

    def beside_x(i, carry):
        fill(i, [pick(odd_x, xnear[c, i], xfar[c, i]) for c in range(4)])
        fill(i + W + 16, [pick(odd_x, xfar[c, i], xnear[c, i]) for c in range(4)])
        return carry

    lax.fori_loop(0, W, beside_x, 0)
    second = (rows_of((8, 128)) >= 4).astype(jnp.int32)
    low_in, high_in = gy > 0, gy < gy_n - 1

    def beside_y(j, carry):
        inside = x_inside(2 * j + second)
        low = values([pick(odd_y, ynear[c, j], yfar[c, j]) for c in range(4)], inside & low_in)
        high = values([pick(odd_y, yfar[c, j], ynear[c, j]) for c in range(4)], inside & high_in)
        for c in range(4):
            for t in range(2):
                pq[2 * j + t, c, pl.ds(4, 4), :] = low[c][4 * t : 4 * t + 4]
                pq[2 * j + t, c, pl.ds(24, 4), :] = high[c][4 * t : 4 * t + 4]
        return carry

    lax.fori_loop(0, NP // 2, beside_y, 0)
    sweep(pq, x2, pq, None, 1, NP - 1, 11)
    lane = lanes_of((8, 128))
    row8 = rows_of((8, 128))

    def residual(i, carry):
        totals = list(carry)
        for row in OWN_GROUPS:
            sums, v = neighbour_sum(x2, None, i, row, lane)
            rows = pl.ds(row - 8, 8)
            g = stiffness_of(f[3, i - W, rows, :])
            d = g * DIAG + MASS_TERM
            for c in range(3):
                load = f[c, i - W, rows, :]
                totals[c] += (load - d * v[c]) + g * sums[c]
                totals[4] += load * load
            totals[3] += g
        return tuple(totals)

    zero = jnp.zeros((8, 128), F32)
    totals = planes(W, W + 16, residual, (zero,) * 5, step=8)
    stacked = zero
    inner = (lane >= 2) & (lane < 126)
    for c in range(5):
        total = jnp.where(inner, totals[c], 0.0) if c < 3 else totals[c]
        stacked = jnp.where(row8 == c, jnp.sum(total, axis=0, keepdims=True), stacked)
    big = (128, 128)
    gather = (rows_of(big) // BLOCK == lanes_of(big) % 8).astype(F32)
    by_cell[...] = jnp.dot(
        stacked, gather, precision=lax.Precision.HIGHEST, preferred_element_type=F32
    )
    sweep(x2, y3, pq, None, 2, NP - 2, 10)


def first_kernel(by_cell, zfar_own, znear_own, zfar, znear, tail, tail_pq, sums_out):
    lane = lanes_of((8, 128))
    row8 = rows_of((8, 128))
    gx, gx_n, _ = position(GX)
    gy, gy_n, _ = position("gy")
    gz, gz_n, odd_z = position(GZ)
    odd_z = odd_z == 1
    x = gx * 16 + lane // W - W
    x_in = (x >= 0) & (x < gx_n * 16)
    y_in = ((row8 >= 4) | (gy > 0)) & ((row8 < 4) | (gy < gy_n - 1))
    z_in = (gz > 0, True, True, gz < gz_n - 1)
    sides = (
        (znear, zfar),
        (znear_own, zfar_own),
        (zfar_own, znear_own),
        (zfar, znear),
    )

    def part(page, c, k):
        when_odd, when_even = sides[page]
        rows = pl.ds(8 * k, 8)
        return pick(odd_z, when_odd[c, rows, :], when_even[c, rows, :])

    for page in range(4):
        for k in range(3):
            g = stiffness_of(part(page, 3, k))
            scale = RELAXATION / (g * DIAG + MASS_TERM)
            inside = x_in
            if page in (0, 3):
                inside = inside & z_in[page]
            if k == 2:
                inside = inside & y_in
            for c in range(4):
                value = jnp.where(inside, (part(page, c, k) if c < 3 else g) * scale, 0.0)
                if k < 2:
                    tail_pq[page, c, pl.ds(8 + 8 * k, 8), :] = value
                else:
                    tail_pq[page, c, pl.ds(4, 4), :] = value[:4]
                    tail_pq[page, c, pl.ds(24, 4), :] = value[4:]
    tail_sweep(tail_pq, tail, tail_pq)
    zero = jnp.zeros((8, 128), F32)
    ends = zero
    for side in range(2):
        page = 1 + side
        here = (lane % W < 2) if side == 0 else (lane % W >= 2)
        totals = [zero] * 3
        for row in OWN_GROUPS:
            sums, v, _, _ = tail_sums(tail, row, 2 * side)
            k = row // 8 - 1
            g = stiffness_of(part(page, 3, k))
            d = g * DIAG + MASS_TERM
            for c in range(3):
                totals[c] += (part(page, c, k) - d * v[1 - side][c]) + g * sums[1 - side][c]
        for c in range(3):
            total = jnp.sum(jnp.where(here, totals[c], 0.0), axis=0, keepdims=True)
            ends = jnp.where(row8 == 3 * side + c, total, ends)
    ends = jnp.where((lane >= W * W) & (lane < W * (W + 16)), ends, 0.0)
    by_end = jnp.sum(ends, axis=1, keepdims=True)
    low_end = (lane % 8 == 0) & (lane // 8 == row8) & (row8 < 3)
    high_end = (lane % 8 == 7) & (lane // 8 + 3 == row8) & (row8 < 6)
    slot = jnp.where(lane // 8 == row8, by_cell[...], 0.0) + jnp.where(
        low_end | high_end, by_end, 0.0
    )
    sums_out[...] = jnp.broadcast_to(jnp.sum(slot, axis=0, keepdims=True), sums_out.shape)


def coarse_solve(load, mean, gx_n, gy_n, gz_n):
    shape = load[0].shape
    n = shape[1]
    lane = lanes_of(shape)
    row = rows_of(shape)
    sx, sy = gy_n * gz_n, gz_n
    x_at, y_at, z_at = lane // sx, lane // sy % gy_n, lane % gz_n

    def shift(v, step, at, count):
        up = jnp.where(at < count - 1, pltpu.roll(v, n - step, 1), 0.0)
        down = jnp.where(at > 0, pltpu.roll(v, step, 1), 0.0)
        return up, down

    def shift_z(v):
        up = pltpu.roll(v, 7, 0)
        down = pltpu.roll(v, 1, 0)
        next_up = jnp.where(z_at < gz_n - 1, pltpu.roll(up, n - 1, 1), 0.0)
        next_down = jnp.where(z_at > 0, pltpu.roll(down, 1, 1), 0.0)
        return jnp.where(row == 7, next_up, up), jnp.where(row == 0, next_down, down)

    shifts = (
        lambda v: shift(v, sx, x_at, gx_n),
        lambda v: shift(v, sy, y_at, gy_n),
        shift_z,
    )
    coefficient = BLOCK**2 * mean
    scale = RELAXATION / (coefficient * DIAG + BLOCK**3 * MASS_TERM)
    p = [scale * value for value in load]
    q = scale * coefficient

    def step(_, w):
        pairs = [[shifts[b](w[a]) for b in range(3)] for a in range(3)]
        diffs = [pairs[a][a][0] - pairs[a][a][1] for a in range(3)]
        out = []
        for a in range(3):
            total = 0.0
            for b in range(3):
                both = pairs[a][b][0] + pairs[a][b][1]
                total = total + (OWN * both if a == b else both)
            others = [diffs[b] for b in range(3) if b != a]
            up, down = shifts[a](others[0] + others[1])
            out.append(KEEP * w[a] + p[a] + q * (total + MIX * (up - down)))
        return tuple(out)

    w = tuple(p)
    for k in range(COARSE - 1):
        w = step(k, w)
    return w


def second_kernel(
    every,
    y3,
    tail2,
    pq,
    tail_pq,
    f,
    out,
    sum_out,
    load_out,
    x3,
    x4,
    tail3,
    tail4,
    w_ref,
    n_ref,
    edges,
    out_sem,
):
    gx, gx_n, _ = position(GX)
    gy, gy_n, _ = position("gy")
    gz, gz_n, _ = position(GZ)
    me = (gx * gy_n + gy) * gz_n + gz
    lane = lanes_of((8, 128))
    row8 = rows_of((8, 128))
    cells = jnp.transpose(every[...])
    load = [cells[8 * c : 8 * c + 8] for c in range(3)]
    mean = cells[24:32] * (1.0 / BLOCK**3)
    load_out[...] = cells[32:40]
    w = coarse_solve(load, mean, gx_n, gy_n, gz_n)
    n = gx_n * gy_n * gz_n
    centre = n // 2
    own_cells = (lane // BLOCK == row8).astype(F32)
    line = lane[:1]
    cell_of = ((7, -1), (0, 0), (7, 0), (0, 1))
    spans = ((4, 4), (8, 16), (24, 4))
    x_cell_in = (gx > 0, True, gx < gx_n - 1)
    y_cell_in = (gy > 0, True, gy < gy_n - 1)
    for c in range(3):
        turned = pltpu.roll(w[c], (centre + n - me) % n, 1)

        def column(dx, dy):
            return centre + (dx - 1) * gy_n * gz_n + (dy - 1) * gz_n

        for dy in range(3):
            first, size = spans[dy]
            for dx in range(3):
                j = column(dx, dy)
                main = jnp.sum(turned[:, j : j + 1] * own_cells, axis=0, keepdims=True)
                main = jnp.where(x_cell_in[dx] & y_cell_in[dy], main, 0.0)
                for k in range(3 * dx, 3 * dx + 3):
                    w_ref[k, c, pl.ds(first, size), :] = jnp.broadcast_to(main, (size, 128))
            for page in range(4):
                k, dz = cell_of[page]
                here = [
                    jnp.broadcast_to(
                        turned[k : k + 1, column(dx, dy) + dz : column(dx, dy) + dz + 1], (1, 128)
                    )
                    for dx in range(3)
                ]
                value = jnp.where(
                    line < W * W, here[0], jnp.where(line < W * (W + 16), here[1], here[2])
                )
                rows = pl.ds(first, size)
                inside = tail_pq[page, 3, rows, :] > 0.0
                tail3[page, c, rows, :] = tail2[page, c, rows, :] + jnp.where(inside, value, 0.0)

    tail_sweep(tail3, tail4, tail_pq)
    for k in range(1, 8):
        for row in GROUPS:
            sums, _ = neighbour_sum(w_ref, None, k, row, lane)
            for c in range(3):
                n_ref[k, c, pl.ds(row, 8), :] = sums[c]
    ends = (lane < 2) | (lane >= 126)
    for row in GROUPS:
        for c in range(3):
            rows = pl.ds(row, 8)
            edges[c, rows, :] = jnp.where(
                lane % W < 2, tail4[1, c, rows, :], pltpu.roll(tail4[2, c, rows, :], 128 - W, 1)
            )

    def correct(i, carry):
        k = jnp.minimum(i - 1, W) + jnp.maximum(i - W - 14, 0)
        for row in GROUPS:
            rows = pl.ds(row, 8)
            q = pq[i, 3, rows, :]
            for c in range(3):
                edge = pltpu.roll(edges[c, rows, :], 128 - W * i, 1)
                value = y3[i, c, rows, :] + KEEP * w_ref[k, c, rows, :] + q * n_ref[k, c, rows, :]
                x4[i, c, rows, :] = jnp.where(ends, edge, value)
        return carry

    planes(2, NP - 2, correct)
    tail_sweep(tail4, tail3, tail_pq, edges, True)
    sweep(x4, x3, pq, edges, 3, NP - 3, 6)
    copies = [
        pltpu.make_async_copy(
            x3.at[pl.ds(W, 16), c, pl.ds(8, 16), :], out.at[c], out_sem.at[c]
        )
        for c in range(3)
    ]
    for copy in copies:
        copy.start()
    edges_only(tail3, edges)

    def residual(i, total):
        for row in OWN_GROUPS:
            sums, v = neighbour_sum(x3, edges, i, row, lane)
            rows = pl.ds(row - 8, 8)
            g = stiffness_of(f[3, i - W, rows, :])
            d = (g * DIAG + MASS_TERM) * (1.0 / RELAXATION)
            q = pq[i, 3, pl.ds(row, 8), :]
            for c in range(3):
                p = pq[i, c, pl.ds(row, 8), :]
                r = d * ((p - RELAXATION * v[c]) + q * sums[c])
                total += r * r
        return total

    total = planes(W, W + 16, residual, jnp.zeros((8, 128), F32), step=8)
    sum_out[...] = jnp.broadcast_to(jnp.sum(total, axis=0, keepdims=True), sum_out.shape)
    for copy in copies:
        copy.wait()


def swaps(far_send, near_send, axis):
    count = lax.axis_size(axis)
    near = [(i, i ^ 1) for i in range(count)]
    far = [(i, ((i ^ 1) + (2 if i % 2 else -2)) % count) for i in range(count)]
    return lax.ppermute(far_send, axis, far), lax.ppermute(near_send, axis, near)


VMEM = pl.BlockSpec(memory_space=pltpu.VMEM)
SMEM = pl.BlockSpec(memory_space=pltpu.SMEM)
HBM = pl.BlockSpec(memory_space=pltpu.HBM)


def call(kernel, shapes, arguments, mib, scratch=(), source=VMEM, target=VMEM):
    shapes = [jax.ShapeDtypeStruct(shape, F32) for shape in shapes]
    return pl.pallas_call(
        kernel,
        out_shape=tuple(shapes),
        in_specs=[source] * len(arguments),
        out_specs=target if isinstance(target, tuple) else (target,) * len(shapes),
        scratch_shapes=[pltpu.VMEM(s, F32) if isinstance(s, tuple) else s for s in scratch],
        compiler_params=pltpu.CompilerParams(vmem_limit_bytes=mib << 20),
    )(*arguments)


def norms_kernel(count, load_parts, residual_parts, out):
    for k, parts in enumerate((load_parts, residual_parts)):
        line = jnp.sum(parts[...], axis=0, keepdims=True)
        total = jnp.sum(line, axis=1, keepdims=True)
        out[k] = jnp.sqrt(total * (1.0 / count))[0, 0]


def on_device(right_side, damage):
    n = lax.axis_size(ALL)
    slab = (4, W, 16, 128)
    f, *x_sends = call(
        x_pack_kernel,
        ((4, 16, 16, 128), slab, slab),
        tuple(pltpu.with_memory_space_constraint(x, pltpu.HBM) for x in (right_side, damage)),
        8,
        (
            pltpu.VMEM((16, 16, 128), jnp.int32),
            pltpu.SemaphoreType.DMA(()),
            pltpu.SemaphoreType.DMA(()),
        ),
        source=HBM,
    )
    x_pieces = swaps(*x_sends, GX)
    slab = (4, NP // 2, 8, 128)
    y_sends = call(y_pack_kernel, (slab, slab), (f, *x_pieces), 8)
    y_pieces = swaps(*y_sends, "gy")
    pieces = (f, *x_pieces, *y_pieces)
    side = (4, NP, 128)
    own_side = (4, 16, 128)
    own_sends = call(z_pack_own_kernel, (own_side, own_side), (f, *x_pieces), 8)
    z_sends = call(z_pack_kernel, (side, side), (*y_pieces, *own_sends), 8)
    z_pieces = swaps(*z_sends, GZ)
    field = (NP, 4, ROWS, 128)
    tails = (4, 4, ROWS, 128)
    edges = (4, ROWS, 128)
    pq, y3, by_cell = call(main_kernel, (field, field, (8, 128)), pieces, 12, (field,))
    tail, tail_pq, sums = call(
        first_kernel, (tails, tails, (n, 128)), (by_cell, *z_sends, *z_pieces), 8
    )
    every = lax.all_to_all(sums, ALL, 0, 0, tiled=True)
    displacement, partial_sums, load_sums = call(
        second_kernel,
        (right_side.shape, (n, 128), (8, n)),
        (every, y3, tail, pq, tail_pq, f),
        20,
        (
            *(field, field, tails, tails),
            *((12, 4, ROWS, 128), (12, 4, ROWS, 128), edges),
            pltpu.SemaphoreType.DMA((3,)),
        ),
        target=(HBM, VMEM, VMEM),
    )
    partial_sums = lax.all_to_all(partial_sums, ALL, 0, 0, tiled=True)
    (norms,) = call(
        functools.partial(norms_kernel, right_side.size * n), ((2,),), (load_sums, partial_sums), 2, target=SMEM
    )
    return (displacement, norms)


def solution(mesh):
    torus = Mesh(mesh.devices.reshape(4, 2, mesh.shape["gy"], 2, 4), ALL)
    placed = (P(None, GX, "gy", GZ), P(GX, "gy", GZ))
    return jax.shard_map(
        on_device,
        mesh=torus,
        in_specs=placed,
        out_specs=(P(None, GX, "gy", GZ), P()),
        check_vma=False,
    )
```
